32 devices in a mesh: group: 2 (over y), gx: 4 (over x, core), gy: 4 (over z).
Axes of the slice: x: 2, y: 2, z: 4, core: 2. Of those that a mesh axis runs over, the one named last changes fastest.
Arguments:
- pressure: float32 [192, 64, 768], P(('group', 'gx'), 'gy'), parts along dimension 0, may hold values from -6 to 6
- pressure_prev: float32 [192, 64, 768], P(('group', 'gx'), 'gy'), parts along dimension 0, may hold values from -6 to 6
- courant: float32 [192, 64, 768], P(('group', 'gx'), 'gy'), parts along dimension 0, may hold values from 0.05 to 0.3
- nonlinearity: float32 [192, 64, 768], P(('group', 'gx'), 'gy'), parts along dimension 0, may hold values from 0.03 to 0.3
- absorption: float32 [192, 64, 768], P(('group', 'gx'), 'gy'), parts along dimension 0, may hold values from 0.2 to 2
- own_map: int32 [96, 32], P(('group', 'gx'), 'gy'), parts along dimension 0, may hold values from 0 to 16, as said below
- slot_table: int32 [96, 32], P(('group', 'gx'), 'gy'), parts along dimension 0, may hold values from 0 to 511
- displacement: float32 [128, 128, 384], P(('group', 'gx'), 'gy'), parts along dimension 0, may hold values from -6 to 6
- displacement_prev: float32 [128, 128, 384], P(('group', 'gx'), 'gy'), parts along dimension 0, may hold values from -6 to 6
- layer_labels: int32 [128, 128, 384], P(('group', 'gx'), 'gy'), parts along dimension 0, may hold values from 0 to 3
- shear_table: float32 [8], P('group'), parts along dimension 0, may hold values from 0.05 to 0.15
- viscosity_table: float32 [8], P('group'), parts along dimension 0, may hold values from 0.01 to 0.06
Outputs:
- pressure_mid: float32 [192, 64, 768], P(('group', 'gx'), 'gy'), parts along dimension 0
- pressure_new: float32 [192, 64, 768], P(('group', 'gx'), 'gy'), parts along dimension 0
- tissue_force: float32 [128, 128, 384], P(('group', 'gx'), 'gy'), parts along dimension 0
- displacement_mid: float32 [128, 128, 384], P(('group', 'gx'), 'gy'), parts along dimension 0
- displacement_new: float32 [128, 128, 384], P(('group', 'gx'), 'gy'), parts along dimension 0
The draws below stay inside these ranges and needn't reach their ends.
There are 2 independent parts, one for each index of `group`. The reference program is written for one: setup_inputs(seed, part) draws one part's arguments, and reference() takes and returns one part's arrays. A program takes and returns all parts, laid end to end along the dimension named above; each array names one. Nothing has to cross between parts.
Inputs may be any that keep to these rules, and one draw needn't show every extreme that they name: `own_map`: A value below 16 names tissue block (v // 4, v % 4); 16 marks a line outside the focal zone. Among the lines of one device's block of the map, at most 6 name any one tissue block, and exactly 6 do for some block in every draw.
All inputs are finite; a program needn't handle non-finite values.
Results may differ from the reference program's by a relative error of at most 0.0003.
Values sent between devices are 32-bit elements; how exact they have to be, the bound alone decides.
A program may use at most 64 MiB of HBM per device.

```python
import math
import jax
import jax.numpy as jnp
from jax import lax

BZ = 24
CX = 16
NY = 768
RX = 16
RY = 32
LAYERS = 4
TZ = 384
NZ = 96
NX = 64
TX = 64
TY = 128
TROWS = 4
TCOLS = 4
TILES = 16
CAP = 6


def focal_routing(key):
    keys = jax.random.split(jax.random.fold_in(key, 7), 2)
    outside_row = jax.random.randint(keys[0], (), 0, TROWS)
    offsets = jax.random.randint(keys[1], (TILES,), 0, TILES)
    depth = BZ // 2
    across = CX // 2
    line_z = jnp.arange(NZ // 2, dtype=jnp.int32)[:, None]
    line_x = jnp.arange(NX // 2, dtype=jnp.int32)[None, :]
    source_row = line_z // depth
    source_col = line_x // across
    local = line_z % depth * across + line_x % across
    group_index = local // CAP
    source = source_row * TCOLS + source_col
    focal = source_row != outside_row
    target = (offsets[source] + group_index) % TILES
    return jnp.where(focal, target, TILES).astype(jnp.int32)


def draw_own_map(key, part):
    return focal_routing(key)


def plant(array, rng, least, high):
    longest = array.shape.index(max(array.shape))
    spots = []
    for shift in (0, 1):
        where = [jax.random.randint(jax.random.fold_in(rng, axis), (), 0, length) for axis, length in enumerate(array.shape)]
        where[longest] = (where[longest] + shift) % array.shape[longest]
        spots.append(tuple(where))
    return array.at[spots[0]].set(least).at[spots[1]].set(high)


def level_of(own_key, dims, cuts, least, largest):
    loudness, own = 1.0, jax.random.fold_in(own_key, 6)
    for position, blocks in cuts:
        draws = jnp.exp(jax.random.uniform(jax.random.fold_in(own, position), (blocks,), jnp.float32, least / len(cuts), largest / len(cuts)))
        loudness = loudness * jnp.repeat(draws, dims[position] // blocks).reshape([-1 if axis == position else 1 for axis in range(len(dims))])
    return loudness


def scatter_about(own_key, shape, deviation, most, cuts=(), kind=jnp.bfloat16):
    entries = deviation * jax.random.normal(own_key, shape, jnp.float32)
    if cuts:
        entries = entries * level_of(own_key, shape, cuts, -0.22, 0.18)
    return jnp.clip(entries, -most, most).astype(kind)


def setup_inputs(seed: int = 0, part: int = 0) -> dict:
    key_of = jax.random.split(jax.random.key(seed), 13)
    part_keys = jax.random.split(jax.random.fold_in(key_of[12], part), 13)
    pressure = scatter_about(part_keys[0], (NZ, NX, NY), 1.0, 6.0, ((0, 4), (1, 4)), jnp.float32)
    pressure_prev = scatter_about(part_keys[1], (NZ, NX, NY), 1.0, 6.0, ((0, 4), (1, 4)), jnp.float32)
    courant = jnp.clip(jnp.exp(math.log(0.3) - 1.7917595 * jax.random.uniform(part_keys[2], (NZ, NX, NY), jnp.float32) ** level_of(part_keys[2], (NZ, NX, NY), ((0, 4), (1, 4)), -0.2, 0.2)), 0.05, 0.3)
    nonlinearity = jnp.clip(jnp.exp(math.log(0.3) - 2.3025852 * jax.random.uniform(part_keys[3], (NZ, NX, NY), jnp.float32) ** level_of(part_keys[3], (NZ, NX, NY), ((0, 4), (1, 4)), -0.2, 0.2)), 0.03, 0.3)
    absorption = jnp.clip(jnp.exp(math.log(2.0) - 2.3025851 * jax.random.uniform(part_keys[4], (NZ, NX, NY), jnp.float32) ** level_of(part_keys[4], (NZ, NX, NY), ((0, 4), (1, 4)), -0.2, 0.2)), 0.2, 2.0)
    own_map = draw_own_map(jax.random.fold_in(jax.random.fold_in(key_of[12], part), 71), part)
    slot_table = plant(jax.random.randint(part_keys[6], (NZ // 2, NX // 2), 0, RX * RY), jax.random.fold_in(part_keys[6], 1), 0, (RX * RY) - 1).astype(jnp.int32)
    displacement = scatter_about(part_keys[7], (TX, TY, TZ), 1.0, 6.0, ((0, 4), (1, 4)), jnp.float32)
    displacement_prev = scatter_about(part_keys[8], (TX, TY, TZ), 1.0, 6.0, ((0, 4), (1, 4)), jnp.float32)
    layer_labels = plant(jax.random.randint(part_keys[9], (TX, TY, TZ), 0, LAYERS), jax.random.fold_in(part_keys[9], 1), 0, LAYERS - 1).astype(jnp.int32)
    shear_table = jnp.clip(jnp.exp(jax.random.uniform(part_keys[10], (LAYERS,), jnp.float32, math.log(0.05), math.log(0.15))), 0.05, 0.15)
    viscosity_table = jnp.clip(jnp.exp(jax.random.uniform(part_keys[11], (LAYERS,), jnp.float32, math.log(0.01), math.log(0.06))), 0.01, 0.06)
    return dict(pressure=pressure, pressure_prev=pressure_prev, courant=courant, nonlinearity=nonlinearity, absorption=absorption, own_map=own_map, slot_table=slot_table, displacement=displacement, displacement_prev=displacement_prev, layer_labels=layer_labels, shear_table=shear_table, viscosity_table=viscosity_table)


def laplace_pad(field):
    padded = jnp.pad(field, 1)
    total = padded[2:, 1:-1, 1:-1] + padded[:-2, 1:-1, 1:-1]
    total = total + padded[1:-1, 2:, 1:-1] + padded[1:-1, :-2, 1:-1]
    total = total + padded[1:-1, 1:-1, 2:] + padded[1:-1, 1:-1, :-2]
    return total - 6.0 * field

def acoustic_step(now, before, courant, nonlinearity, absorption):
    return 2.0 * now - before + courant * laplace_pad(now) + nonlinearity * (now * now - before * before) - 0.1 * absorption * (now - before)

def layer_lookup(labels, table):
    result = jnp.zeros(labels.shape, jnp.float32)
    for kind in range(table.shape[0]):
        result = result + jnp.where(labels == kind, table[kind], 0.0)
    return result

def reference(pressure, pressure_prev, courant, nonlinearity, absorption, own_map, slot_table, displacement, displacement_prev, layer_labels, shear_table, viscosity_table):
    pressure_mid = acoustic_step(pressure, pressure_prev, courant, nonlinearity, absorption)
    pressure_new = acoustic_step(pressure_mid, pressure, courant, nonlinearity, absorption)
    force = 0.1 * absorption * (pressure_mid * pressure_mid + pressure_new * pressure_new) * lax.rsqrt(courant)
    coarse = force.reshape(NZ // 2, 2, NX // 2, 2, TZ, 2).sum(axis=(1, 3, 5)) * 0.125
    rows = own_map // TCOLS * RX + slot_table // RY
    cols = own_map % TCOLS * RY + slot_table % RY
    target = jnp.where(own_map < TILES, rows * TY + cols, TX * TY).astype(jnp.int32)
    summed = jax.ops.segment_sum(coarse.reshape(-1, TZ), target.reshape(-1), num_segments=TX * TY + 1)
    tissue_force = summed[:-1].reshape(TX, TY, TZ)
    shear = layer_lookup(layer_labels, shear_table)
    viscosity = layer_lookup(layer_labels, viscosity_table)

    def elastic_step(now, before):
        return 2.0 * now - before + shear * laplace_pad(now) + viscosity * laplace_pad(now - before) + 0.25 * tissue_force
    displacement_mid = elastic_step(displacement, displacement_prev)
    displacement_new = elastic_step(displacement_mid, displacement)
    return (pressure_mid, pressure_new, tissue_force, displacement_mid, displacement_new)
```

```python
import functools

import jax
import jax.numpy as jnp
from jax import lax
from jax.experimental import pallas as pl
from jax.experimental.pallas import tpu as pltpu
from jax.sharding import PartitionSpec as P

MESH = pl.DeviceIdType.MESH
F32 = jnp.float32
BF16 = jnp.bfloat16


def iota(shape, dim):
    return lax.broadcasted_iota(jnp.int32, shape, dim)


def split(x):
    high = x.astype(BF16)
    low = (x - high.astype(F32)).astype(BF16)
    return high, low


def dot(a, b):
    return jnp.dot(a, b, preferred_element_type=F32)


def laplace(centre, up, down, left=0.0, right=0.0):
    rows, lanes = centre.shape
    row, lane = iota(centre.shape, 0), iota(centre.shape, 1)
    xm = jnp.where(row == 0, left, pltpu.roll(centre, 1, 0))
    xp = jnp.where(row == rows - 1, right, pltpu.roll(centre, rows - 1, 0))
    ym = jnp.where(lane == 0, 0.0, pltpu.roll(centre, 1, 1))
    yp = jnp.where(lane == lanes - 1, 0.0, pltpu.roll(centre, lanes - 1, 1))
    if up is None:
        beside = down
    elif down is None:
        beside = up
    else:
        beside = up + down
    return (beside + (xm + xp)) + ((ym + yp) - 6.0 * centre)


class Faces:
    def __init__(self, axis, pieces, halo, send, recv, base):
        size, index = lax.axis_size(axis), lax.axis_index(axis)
        self.halo = halo
        self.has_next, self.has_prev = index < size - 1, index > 0
        self.up, self.down = [], []
        for i, (first, last, part) in enumerate(pieces):
            at = base + 2 * i
            self.up.append(pltpu.make_async_remote_copy(
                src_ref=last, dst_ref=part(halo, 0), send_sem=send.at[at], recv_sem=recv.at[at],
                device_id={axis: lax.rem(index + 1, size)}, device_id_type=MESH))
            self.down.append(pltpu.make_async_remote_copy(
                src_ref=first, dst_ref=part(halo, 1), send_sem=send.at[at + 1], recv_sem=recv.at[at + 1],
                device_id={axis: lax.rem(index + size - 1, size)}, device_id_type=MESH))

    def clear(self):
        @pl.when(jnp.logical_not(self.has_prev))
        def _():
            self.halo[0] = jnp.zeros(self.halo.shape[1:], F32)

        @pl.when(jnp.logical_not(self.has_next))
        def _():
            self.halo[1] = jnp.zeros(self.halo.shape[1:], F32)

    def start(self, i=0):
        pl.when(self.has_next)(self.up[i].start)
        pl.when(self.has_prev)(self.down[i].start)

    def wait(self, i=0):
        pl.when(self.has_prev)(self.up[i].wait_recv)
        pl.when(self.has_next)(self.down[i].wait_recv)

    def wait_send(self):
        @pl.when(self.has_next)
        def _():
            for copy in self.up:
                copy.wait_send()

        @pl.when(self.has_prev)
        def _():
            for copy in self.down:
                copy.wait_send()


def kernel(
    capacity, slots, width,
    p_in, q_in, c_in, n_in, a_in, own_in, slot_in, u_in, w_in, k_in, shear_in, viscosity_in,
    pm, pn, tf, um, un, both, hz_out, hx_out,
    p, q, c, n, a, u, w, k, own, slot, shear_table, viscosity_table, load,
    fz_p, fx_p, fx_c, fx_a, fx_m, fx_n, fz_e, fx_e,
    hz_p, hx_p, hz_m, hx_m, hz_u, hx_u, hz_w, hx_w, hz_e, hx_e,
    rest, paired, gain, packed, got, packed_places, got_places,
    send, recv, line_send, line_recv, place_send, place_recv,
):
    planes, rows, lateral = p.shape
    tile_rows, tile_cols, tile_depth = u.shape
    kinds = shear_table.shape[0]
    half = width // 2
    chunks = lateral // width
    gx, gy = lax.axis_size("gx"), lax.axis_size("gy")
    blocks = gx * gy
    me = lax.axis_index("gx") * gy + lax.axis_index("gy")

    barrier = pltpu.get_barrier_semaphore()

    def greet(d, carry):
        other = lax.rem(me + d, blocks)
        pl.semaphore_signal(
            barrier, inc=1, device_id={"gx": other // gy, "gy": lax.rem(other, gy)}, device_id_type=MESH)
        return carry

    cuts = 3 if planes % 3 == 0 else 1
    step = planes // cuts

    def load_of(pairs, base):
        return [pltpu.make_async_copy(s, d, load.at[base + i]) for i, (s, d) in enumerate(pairs)]

    faces_in = load_of((
        (p_in.at[:, 0, :], fx_p.at[0]), (p_in.at[:, rows - 1, :], fx_p.at[1]),
        (p_in.at[0], fz_p.at[0]), (p_in.at[planes - 1], fz_p.at[1])), 0)
    waves_in = [load_of([(s.at[pl.ds(i * step, step)], d.at[pl.ds(i * step, step)]) for s, d in (
        (p_in, p), (q_in, q), (c_in, c), (n_in, n), (a_in, a))], 4 + 5 * i) for i in range(cuts)]
    base = 4 + 5 * cuts
    table_in = load_of(((own_in, own), (slot_in, slot)), base)
    sides_in = load_of((
        (c_in.at[:, 0, :], fx_c.at[0]), (c_in.at[:, rows - 1, :], fx_c.at[1]),
        (a_in.at[:, 0, :], fx_a.at[0]), (a_in.at[:, rows - 1, :], fx_a.at[1])), base + 2)
    cells_in = load_of((
        (u_in, u), (w_in, w), (k_in, k), (shear_in, shear_table), (viscosity_in, viscosity_table)), base + 6)

    for copy in faces_in:
        copy.start()
    lax.fori_loop(1, blocks, greet, 0)
    for copy in table_in:
        copy.start()
    for group in waves_in:
        for copy in group:
            copy.start()
    for copy in sides_in + cells_in:
        copy.start()

    def lanes(i):
        return slice(i * width, (i + 1) * width)

    def depths(i):
        return slice(i * half, (i + 1) * half)

    def whole(halo, side):
        return halo.at[side]

    def cut(at):
        return lambda halo, side: halo.at[side, :, at]

    def cut_all(first, last, at):
        return [(first.at[:, at(i)], last.at[:, at(i)], cut(at(i))) for i in range(chunks)]

    p_z = Faces("gx", cut_all(fz_p.at[0], fz_p.at[1], lanes), hz_p, send, recv, 0)
    p_x = Faces("gy", cut_all(fx_p.at[0], fx_p.at[1], lanes), hx_p, send, recv, 2 * chunks)
    m_z = Faces("gx", cut_all(pm.at[0], pm.at[planes - 1], lanes), hz_m, send, recv, 4 * chunks)
    m_x = Faces("gy", cut_all(fx_m.at[0], fx_m.at[1], lanes), hx_m, send, recv, 6 * chunks)
    e_z = Faces("gx", cut_all(fz_e.at[0], fz_e.at[1], depths), hz_e, send, recv, 8 * chunks)
    e_x = Faces("gy", cut_all(fx_e.at[0], fx_e.at[1], depths), hx_e, send, recv, 10 * chunks)
    rest_at = 12 * chunks
    u_z = Faces("gx", [(u_in.at[0], u_in.at[tile_rows - 1], whole)], hz_u, send, recv, rest_at)
    u_x = Faces("gy", [(u_in.at[:, 0, :], u_in.at[:, tile_cols - 1, :], whole)], hx_u, send, recv, rest_at + 2)
    w_z = Faces("gx", [(w_in.at[0], w_in.at[tile_rows - 1], whole)], hz_w, send, recv, rest_at + 4)
    w_x = Faces("gy", [(w_in.at[:, 0, :], w_in.at[:, tile_cols - 1, :], whole)], hx_w, send, recv, rest_at + 6)
    every = (p_z, p_x, m_z, m_x, u_z, u_x, w_z, w_x, e_z, e_x)

    for copy in faces_in:
        copy.wait()
    pl.semaphore_wait(barrier, blocks - 1)
    for i in range(chunks):
        p_x.start(i)
        p_z.start(i)
    for item in (u_x, w_x, u_z, w_z):
        item.start()
    for item in every:
        item.clear()

    for copy in table_in:
        copy.wait()
    lines_x, lines_z = own.shape
    count = lines_z * rows
    total = count + 2 * planes
    padded = -(-total // 128) * 128

    def line_of(column):
        beyond = column - count
        side = jnp.where(beyond >= planes, 1, 0)
        x = jnp.where(column < count, lax.rem(column, rows) // 2, side * (lines_x - 1))
        z = jnp.where(column < count, column // rows, (beyond - side * planes) // 2)
        return z, x

    def along_lanes(table):
        z_of, x_of = line_of(iota((lines_x, padded), 1))
        here = x_of == iota((lines_x, padded), 0)
        result = jnp.zeros((lines_x, padded), F32)
        for z in range(lines_z):
            result = result + jnp.where(here & (z_of == z), table[:, z:z + 1], 0.0)
        return jnp.sum(result, axis=0, keepdims=True)

    owners = own[...].astype(F32)
    owner_lane = along_lanes(owners)
    owner_row = jnp.transpose(jnp.broadcast_to(owner_lane, (128, padded)))[:count, :1]
    owner_lane = owner_lane[:, :total]
    place_lane = along_lanes(slot[...].astype(F32))[:, :total]
    z_of, x_of = line_of(iota((count, total), 1))
    earlier = iota((count, total), 0) // 2 < z_of * lines_x + x_of
    rank = 0.5 * jnp.sum(
        jnp.where((owner_row == owner_lane) & earlier, 1.0, 0.0), axis=0, keepdims=True)
    target = owner_lane * float(slots) + rank
    match = iota((blocks * slots, total), 0).astype(F32) == target
    column = iota((blocks * slots, total), 1)
    counted = (lax.rem(column, 2) == 0) & (column < count)
    places = jnp.sum(jnp.where(match & counted, place_lane + 1.0, 0.0), axis=1, keepdims=True)
    aligned = lax.rem(iota((blocks * slots, 128), 0), slots) == lax.rem(iota((blocks * slots, 128), 1), slots)
    places = jnp.where(aligned, places, 0.0).reshape(blocks, slots, 128)
    packed_places[...] = jnp.sum(places, axis=1, keepdims=True)
    match = jnp.where(match, 1.0, 0.0).astype(BF16)

    def at_block(other):
        return {"gx": other // gy, "gy": lax.rem(other, gy)}

    def each(start):
        lax.fori_loop(1, blocks, lambda d, carry: (start(lax.rem(me + d, blocks)), carry)[1], 0)

    def place_copy(source, target_ref, device):
        return pltpu.make_async_remote_copy(
            src_ref=source, dst_ref=target_ref, send_sem=place_send.at[0], recv_sem=place_recv.at[0],
            device_id=at_block(device), device_id_type=MESH)

    def line_copy(i, source, target_ref, device):
        return pltpu.make_async_remote_copy(
            src_ref=source, dst_ref=target_ref, send_sem=line_send.at[i], recv_sem=line_recv.at[i],
            device_id=at_block(device), device_id_type=MESH)

    used = pl.ds(0, capacity)
    others = pl.ds(0, blocks - 1)

    def start_places():
        each(lambda other: place_copy(packed_places.at[other], got_places.at[me], other).start())
        got_places[me] = packed_places[me]

    def start_lines(i):
        each(lambda other: line_copy(
            i, packed.at[i, other, used], got.at[i, me, used], other).start())
        got[i, me] = packed[i, me]

    all_places = place_copy(packed_places.at[others], got_places.at[others], 0)
    all_lines = [line_copy(i, packed.at[i, others, used], got.at[i, others, used], 0) for i in range(chunks)]

    start_places()

    def wave(now, before, lap, z):
        return (2.0 * now - before + c[z] * lap + n[z] * (now * now - before * before)
                - 0.1 * a[z] * (now - before))

    def first(z, up, down):
        now = p[z]
        mid = wave(now, q[z], laplace(now, up, down), z)
        pm[z] = mid
        fx_m[0, pl.ds(z, 1), :] = mid[:1]
        fx_m[1, pl.ds(z, 1), :] = mid[-1:]

    for i, group in enumerate(waves_in):
        for copy in group:
            copy.wait()
        low, high = i * step - 1, (i + 1) * step - 1
        if i == 0:
            first(0, None, p[1])
            low = 1
        if i == cuts - 1:
            high = planes - 1
        lax.fori_loop(low, high, lambda z, carry: (first(z, p[z - 1], p[z + 1]), carry)[1], 0)
        if i == cuts - 1:
            first(planes - 1, p[planes - 2], None)
    for copy in sides_in:
        copy.wait()

    for i in range(chunks):
        at = lanes(i)
        p_x.wait(i)
        p_z.wait(i)
        top = c[0, :, at] * hz_p[0, :, at]
        bottom = c[planes - 1, :, at] * hz_p[1, :, at]
        pm[0, :, at] = pm[0, :, at] + top
        pm[planes - 1, :, at] = pm[planes - 1, :, at] + bottom
        z = iota((planes, width), 0)
        for side, row in ((0, 0), (1, rows - 1)):
            extra = fx_c[side, :, at] * hx_p[side, :, at]
            extra = extra + jnp.where(z == 0, top[row:row + 1], 0.0)
            extra = extra + jnp.where(z == planes - 1, bottom[row:row + 1], 0.0)
            mid = fx_m[side, :, at] + extra
            fx_m[side, :, at] = mid
            pm[:, row, at] = mid
        m_x.start(i)
        m_z.start(i)

    def second(z, up, down):
        now = pm[z]
        new = wave(now, p[z], laplace(now, up, down), z)
        pn[z] = new
        fx_n[0, pl.ds(z, 1), :] = new[:1]
        fx_n[1, pl.ds(z, 1), :] = new[-1:]
        return 0.1 * a[z] * (now * now + new * new) * lax.rsqrt(c[z])

    def pair_at(i):
        return pl.ds(pl.multiple_of(i * rows, rows), rows)

    paired[pair_at(0), :] = second(0, None, pm[1]) + second(1, pm[0], pm[2])
    last = planes // 2 - 1

    def two(i, carry):
        z = 2 * i
        paired[pair_at(i), :] = second(z, pm[z - 1], pm[z + 1]) + second(z + 1, pm[z], pm[z + 2])
        return carry

    lax.fori_loop(1, last, two, 0)
    paired[pair_at(last), :] = second(planes - 2, pm[planes - 3], pm[planes - 1]) + second(
        planes - 1, pm[planes - 2], None)
    gain[...] = 0.1 * fx_a[...] * lax.rsqrt(fx_c[...])

    lanes_two = jnp.where(iota((width, half), 0) // 2 == iota((width, half), 1), 0.125, 0.0).astype(BF16)
    for i in range(chunks):
        at = lanes(i)
        m_x.wait(i)
        m_z.wait(i)
        for side, z, pair in ((0, 0, 0), (1, planes - 1, last)):
            old = pn[z, :, at]
            extra = c[z, :, at] * hz_m[side, :, at]
            new = old + extra
            pn[z, :, at] = new
            fx_n[0, z:z + 1, at] = new[:1]
            fx_n[1, z:z + 1, at] = new[-1:]
            where = slice(pair * rows, (pair + 1) * rows)
            paired[where, at] = paired[where, at] + (
                0.1 * a[z, :, at] * lax.rsqrt(c[z, :, at]) * (extra * (2.0 * old + extra)))
        for side in range(2):
            old = fx_n[side, :, at]
            extra = fx_c[side, :, at] * hx_m[side, :, at]
            fx_n[side, :, at] = old + extra
            paired[count + side * planes:count + (side + 1) * planes, at] = (
                gain[side, :, at] * (extra * (2.0 * old + extra)))
        high, low = split(paired[:, at])
        coarse = dot(high, lanes_two) + dot(low, lanes_two)
        high, low = split(coarse)
        packed[i] = (dot(match, high) + dot(match, low)).reshape(blocks, slots, half)
        start_lines(i)

    for side, row in ((0, 0), (1, rows - 1)):
        pn[:, row, :] = fx_n[side]

    for copy in cells_in:
        copy.wait()
    for item in (u_z, u_x, w_z, w_x):
        item.wait()

    def elastic(z, u_up, u_down, w_up, w_down):
        now, before, kind = u[z], w[z], k[z]
        lap_u = laplace(now, u_up, u_down, hx_u[0, pl.ds(z, 1), :], hx_u[1, pl.ds(z, 1), :])
        lap_w = laplace(before, w_up, w_down, hx_w[0, pl.ds(z, 1), :], hx_w[1, pl.ds(z, 1), :])
        shear, viscosity = jnp.zeros(now.shape, F32), jnp.zeros(now.shape, F32)
        for i in range(kinds):
            shear = jnp.where(kind == i, shear_table[i], shear)
            viscosity = jnp.where(kind == i, viscosity_table[i], viscosity)
        mid = 2.0 * now - before + shear * lap_u + viscosity * (lap_u - lap_w)
        um[z] = mid
        fx_e[0, pl.ds(z, 1), :] = mid[:1]
        fx_e[1, pl.ds(z, 1), :] = mid[-1:]
        rest[z] = now + viscosity * lap_u
        both[z] = shear + viscosity

    elastic(0, hz_u[0], u[1], hz_w[0], w[1])
    elastic(tile_rows - 1, u[tile_rows - 2], hz_u[1], w[tile_rows - 2], hz_w[1])
    lax.fori_loop(1, tile_rows - 1, lambda z, carry: (
        elastic(z, u[z - 1], u[z + 1], w[z - 1], w[z + 1]), carry)[1], 0)

    all_places.wait_recv()
    spread = -(-blocks * slots // 128)
    sources = jnp.concatenate([got_places[:, 0, :]] * spread, axis=1)[:, :blocks * slots]
    mine = iota((blocks, blocks * slots), 1) // slots == iota((blocks, blocks * slots), 0)
    spots = jnp.sum(jnp.where(mine, sources, 0.0), axis=0, keepdims=True) - 1.0
    cells = tile_rows * tile_cols

    def landing_of(cell):
        return jnp.where(cell.astype(F32) == spots, 1.0, 0.0).astype(BF16)

    landing = landing_of(iota((cells, blocks * slots), 0))
    edges = 2 * tile_cols + 2 * tile_rows
    edge = iota((edges, blocks * slots), 0)
    beyond = edge - 2 * tile_cols
    edge_landing = landing_of(jnp.where(
        edge < tile_cols, edge, jnp.where(
            edge < 2 * tile_cols, edge + (cells - 2 * tile_cols), jnp.where(
                beyond < tile_rows, beyond * tile_cols, (beyond - tile_rows) * tile_cols + tile_cols - 1))))
    real = lax.rem(iota((blocks * slots, half), 0), slots) < capacity

    chunk = 4 if tile_rows % 4 == 0 else 1
    for i in range(chunks):
        at = depths(i)
        all_lines[i].wait_recv()
        lines = jnp.where(real, got[i].reshape(blocks * slots, half), 0.0)
        parts = jnp.concatenate(split(lines), axis=1)

        def sums(where):
            result = dot(where, parts)
            return result[:, :half] + result[:, half:]

        edge_force = 0.25 * sums(edge_landing)
        for side, z in ((0, 0), (1, tile_rows - 1)):
            fz_e[side, :, at] = um[z, :, at] + edge_force[side * tile_cols:(side + 1) * tile_cols]
            here = 2 * tile_cols + side * tile_rows
            fx_e[side, :, at] = fx_e[side, :, at] + edge_force[here:here + tile_rows]
        e_x.start(i)
        e_z.start(i)
        for r in range(0, tile_rows, chunk):
            force = sums(landing[r * tile_cols:(r + chunk) * tile_cols]).reshape(chunk, tile_cols, half)
            tf[r:r + chunk, :, at] = force
            um[r:r + chunk, :, at] = um[r:r + chunk, :, at] + 0.25 * force

    def final(z, up, down):
        now = um[z]
        un[z] = 2.0 * now - rest[z] + both[z] * laplace(now, up, down) + 0.25 * tf[z]

    final(0, None, um[1])
    final(tile_rows - 1, um[tile_rows - 2], None)
    lax.fori_loop(1, tile_rows - 1, lambda z, carry: (final(z, um[z - 1], um[z + 1]), carry)[1], 0)

    for item in every[:-2]:
        item.wait_send()
    all_places.wait_send()
    for item in all_lines:
        item.wait_send()
    for i in range(chunks):
        e_z.wait(i)
        e_x.wait(i)
    hz_out[...] = hz_e[...]
    hx_out[...] = hx_e[...]
    e_z.wait_send()
    e_x.wait_send()


def finish(pm, pn, tf, um, partial, both, hz, hx, pm_out, pn_out, tf_out, um_out, un_out, un, sems):
    copies = [pltpu.make_async_copy(s, d, sems.at[i]) for i, (s, d) in enumerate(
        ((pm, pm_out), (pn, pn_out), (tf, tf_out), (um, um_out)))]
    for copy in copies:
        copy.start()
    tile_rows, tile_cols, _ = um.shape

    def final(z, carry):
        scale = both[z]
        row = iota(scale.shape, 0)
        extra = jnp.where(row == 0, hx[0, pl.ds(z, 1), :], 0.0) + jnp.where(
            row == tile_cols - 1, hx[1, pl.ds(z, 1), :], 0.0)
        un[z] = partial[z] + scale * extra
        return carry

    lax.fori_loop(0, tile_rows, final, 0)
    for side, z in ((0, 0), (1, tile_rows - 1)):
        un[z] = un[z] + both[z] * hz[side]
    copies.append(pltpu.make_async_copy(un, un_out, sems.at[4]))
    copies[4].start()
    for copy in copies:
        copy.wait()


def local(pressure, pressure_prev, courant, nonlinearity, absorption, own_map, slot_table,
          displacement, displacement_prev, layer_labels, shear_table, viscosity_table):
    planes, rows, lateral = pressure.shape
    tile = displacement.shape
    blocks = lax.axis_size("gx") * lax.axis_size("gy")
    capacity = max(2, own_map.shape[0] * own_map.shape[1] // blocks)
    slots = -(-capacity // 8) * 8
    width = 256
    chunks = lateral // width
    hbm = pl.BlockSpec(memory_space=pltpu.HBM)
    vmem = pl.BlockSpec(memory_space=pltpu.VMEM)
    wave, cell = pltpu.VMEM(pressure.shape, F32), pltpu.VMEM(tile, F32)

    def along_z(shape):
        return pltpu.VMEM((2,) + shape[1:], F32)

    def along_x(shape):
        return pltpu.VMEM((2, shape[0], shape[2]), F32)

    dma = pltpu.SemaphoreType.DMA
    kinds = shear_table.shape[0]
    table = pltpu.VMEM(own_map.shape[::-1], jnp.int32)
    wave_z, wave_x, cell_z, cell_x = along_z(pressure.shape), along_x(pressure.shape), along_z(tile), along_x(tile)
    lines = pltpu.VMEM((chunks, blocks, slots, width // 2), F32)
    places = pltpu.VMEM((blocks, 1, 128), F32)
    waves = [jax.ShapeDtypeStruct(pressure.shape, F32)] * 2
    cells = [jax.ShapeDtypeStruct(tile, F32)]
    parts = pl.pallas_call(
        functools.partial(kernel, capacity, slots, width),
        out_shape=[wave] * 2 + [cell] * 4 + [cell_z, cell_x],
        in_specs=[hbm] * 12,
        out_specs=[vmem] * 8,
        scratch_shapes=[wave] * 5 + [cell] * 2 + [
            pltpu.VMEM(tile, jnp.int32), table, table,
            pltpu.SMEM((kinds,), F32), pltpu.SMEM((kinds,), F32), dma((32,)),
            wave_z, wave_x, wave_x, wave_x, wave_x, wave_x, cell_z, cell_x,
            wave_z, wave_x, wave_z, wave_x, cell_z, cell_x, cell_z, cell_x, cell_z, cell_x,
            cell, pltpu.VMEM((planes // 2 * rows + 2 * planes, lateral), F32), wave_x,
            lines, lines, places, places,
            dma((12 * chunks + 8,)), dma((12 * chunks + 8,)), dma((chunks,)), dma((chunks,)), dma((1,)), dma((1,))],
        compiler_params=pltpu.CompilerParams(
            collective_id=0, has_side_effects=True, vmem_limit_bytes=58 * 1024 * 1024),
    )(pressure, pressure_prev, courant, nonlinearity, absorption, own_map.T, slot_table.T,
      displacement, displacement_prev, layer_labels, shear_table, viscosity_table)
    return pl.pallas_call(
        finish,
        out_shape=waves + cells * 3,
        in_specs=[vmem] * 8,
        out_specs=[hbm] * 5,
        scratch_shapes=[cell, dma((5,))],
        compiler_params=pltpu.CompilerParams(vmem_limit_bytes=40 * 1024 * 1024),
    )(*parts)


def solution(mesh):
    field = P(("group", "gx"), "gy", None)
    table = P(("group", "gx"), "gy")
    return jax.shard_map(
        local,
        mesh=mesh,
        in_specs=(field,) * 5 + (table,) * 2 + (field,) * 3 + (P("group"),) * 2,
        out_specs=(field,) * 5,
        check_vma=False,
    )
```

```python
import functools

import jax
import jax.numpy as jnp
from jax import lax
from jax.experimental import pallas as pl
from jax.experimental.pallas import tpu as pltpu
from jax.sharding import PartitionSpec as P

MESH = pl.DeviceIdType.MESH
F32 = jnp.float32
BF16 = jnp.bfloat16


def iota(shape, dim):
    return lax.broadcasted_iota(jnp.int32, shape, dim)


def split(x):
    high = x.astype(BF16)
    low = (x - high.astype(F32)).astype(BF16)
    return high, low


def dot(a, b):
    return jnp.dot(a, b, preferred_element_type=F32)


def laplace(centre, up, down, left=0.0, right=0.0):
    rows, lanes = centre.shape
    row, lane = iota(centre.shape, 0), iota(centre.shape, 1)
    xm = jnp.where(row == 0, left, pltpu.roll(centre, 1, 0))
    xp = jnp.where(row == rows - 1, right, pltpu.roll(centre, rows - 1, 0))
    ym = jnp.where(lane == 0, 0.0, pltpu.roll(centre, 1, 1))
    yp = jnp.where(lane == lanes - 1, 0.0, pltpu.roll(centre, lanes - 1, 1))
    if up is None:
        beside = down
    elif down is None:
        beside = up
    else:
        beside = up + down
    return (beside + (xm + xp)) + ((ym + yp) - 6.0 * centre)


class Faces:
    def __init__(self, line, pieces, halo, recv, base):
        self.line, self.halo = line, halo
        self.up, self.down, self.one, self.two = [], [], [], []
        for i, (first, last, part) in enumerate(pieces):
            arrived = recv.at[base + i]
            self.up.append(line.copy(last, part(halo, 0), arrived, True))
            self.down.append(line.copy(first, part(halo, 1), arrived, False))
            self.one.append(line.copy(part(halo, 0), part(halo, 0), arrived, True))
            self.two.append(line.copy(part(halo, slice(None)), part(halo, slice(None)), arrived, True))

    def clear(self):
        @pl.when(jnp.logical_not(self.line.has_prev))
        def _():
            self.halo[0] = jnp.zeros(self.halo.shape[1:], F32)

        @pl.when(jnp.logical_not(self.line.has_next))
        def _():
            self.halo[1] = jnp.zeros(self.halo.shape[1:], F32)

    def start(self, i=0):
        pl.when(self.line.has_next)(self.up[i].start)
        pl.when(self.line.has_prev)(self.down[i].start)

    def wait(self, i=0):
        pl.when(self.line.inside)(self.two[i].wait_recv)
        pl.when(self.line.at_end)(self.one[i].wait_recv)


class Line:
    def __init__(self, axis, sent, token):
        size, self.index = lax.axis_size(axis), lax.axis_index(axis)
        index = self.index
        self.size, self.axis, self.sent, self.token = size, axis, sent, token
        self.next = jnp.where(index == size - 1, 0, index + 1)
        self.prev = jnp.where(index == 0, size - 1, index - 1)
        self.has_next, self.has_prev = index < size - 1, index > 0
        self.inside = self.has_next & self.has_prev
        self.at_end = (index == 0) | (index == size - 1)
        self.low = index < size // 2
        self.neighbours = jnp.where(index < size - 1, 1, 0) + jnp.where(index > 0, 1, 0)

    def copy(self, source, target, arrived, up):
        return pltpu.make_async_remote_copy(
            src_ref=source, dst_ref=target, send_sem=self.sent.at[0 if up else 1], recv_sem=arrived,
            device_id={self.axis: self.next if up else self.prev}, device_id_type=MESH)

    def greet(self, barrier):
        for here, other in ((self.has_next, self.next), (self.has_prev, self.prev)):
            @pl.when(here)
            def _():
                pl.semaphore_signal(barrier, inc=1, device_id={self.axis: other}, device_id_type=MESH)

    def tell_next(self):
        pl.semaphore_signal(self.token.at[0], inc=1, device_id={self.axis: self.next}, device_id_type=MESH)

    def tell_prev(self):
        pl.semaphore_signal(self.token.at[1], inc=1, device_id={self.axis: self.prev}, device_id_type=MESH)

    def open(self):
        pl.when(self.index == 0)(self.tell_next)
        pl.when(self.index == self.size - 1)(self.tell_prev)

    def pass_up(self, where):
        @pl.when(where & self.inside)
        def _():
            pl.semaphore_wait(self.token.at[0], 1)
            self.tell_next()

    def pass_down(self, where):
        @pl.when(where & self.inside)
        def _():
            pl.semaphore_wait(self.token.at[1], 1)
            self.tell_prev()

    def near(self):
        self.pass_up(self.low)
        self.pass_down(jnp.logical_not(self.low))

    def far(self):
        self.pass_up(jnp.logical_not(self.low))
        self.pass_down(self.low)

    def close(self):
        @pl.when(self.index == 0)
        def _():
            pl.semaphore_wait(self.token.at[1], 1)

        @pl.when(self.index == self.size - 1)
        def _():
            pl.semaphore_wait(self.token.at[0], 1)

    def wait_sent(self, ref, size):
        whole = ref.at[0:size]
        pl.when(self.has_next)(self.copy(whole, whole, self.sent.at[0], True).wait_send)
        pl.when(self.has_prev)(self.copy(whole, whole, self.sent.at[0], False).wait_send)


def kernel(
    capacity, slots, width,
    p_in, q_in, c_in, n_in, a_in, own_in, slot_in, u_in, w_in, k_in, shear_in, viscosity_in,
    pm, pn, tf, um, un, both, hz_out, hx_out,
    fields, now_before, k, tables, layers, load,
    faces_p, sides, fx_m, fx_n, fz_e, fx_e,
    hz_p, hx_p, hz_m, hx_m, hz_uw, hx_uw, hz_e, hx_e,
    rest, paired, gain, packed, got,
    sent_z, sent_x, recv, line_send, line_recv, token_z, token_x,
):
    _, planes, rows, lateral = fields.shape
    _, tile_rows, tile_cols, tile_depth = now_before.shape
    kinds = layers.shape[1]
    p, q, c, n, a = (fields.at[i] for i in range(5))
    u, w = now_before.at[0], now_before.at[1]
    own, slot = tables.at[0], tables.at[1]
    fx_p = [faces_p.at[i * planes:(i + 1) * planes] for i in range(2)]
    fz_p = [faces_p.at[2 * planes + i * rows:2 * planes + (i + 1) * rows] for i in range(2)]
    fx_c, fx_a = sides.at[0:2], sides.at[2:4]
    half = width // 2
    chunks = lateral // width
    gx, gy = lax.axis_size("gx"), lax.axis_size("gy")
    blocks = gx * gy
    me_x, me_y = lax.axis_index("gx"), lax.axis_index("gy")
    me = me_x * gy + me_y
    along_gx, along_gy = Line("gx", sent_z, token_z), Line("gy", sent_x, token_x)

    barrier = pltpu.get_barrier_semaphore()
    cuts = 3 if planes % 3 == 0 else 1
    step = planes // cuts

    def loads(at, total, pairs):
        copies = [pltpu.make_async_copy(s, d, load.at[at]) for s, d in pairs]
        return copies, pltpu.make_async_copy(total, total, load.at[at])

    def start(group):
        for copy in group[0]:
            copy.start()

    faces_in = loads(0, faces_p, (
        (p_in.at[:, 0, :], fx_p[0]), (p_in.at[:, rows - 1, :], fx_p[1]),
        (p_in.at[0], fz_p[0]), (p_in.at[planes - 1], fz_p[1])))
    waves_in = []
    for i in range(cuts):
        part = pl.ds(i * step, step)
        waves_in.append(loads(6 + i, fields.at[:, part], [
            (s.at[part], fields.at[j, part]) for j, s in enumerate((p_in, q_in, c_in, n_in, a_in))]))
    tables_in = loads(1, tables, ((own_in, own), (slot_in, slot)))
    sides_in = loads(2, sides, (
        (c_in.at[:, 0, :], sides.at[0]), (c_in.at[:, rows - 1, :], sides.at[1]),
        (a_in.at[:, 0, :], sides.at[2]), (a_in.at[:, rows - 1, :], sides.at[3])))
    cells_in = loads(3, now_before, ((u_in, u), (w_in, w)))
    kinds_in = loads(4, k, ((k_in, k),))
    layers_in = loads(5, layers, ((shear_in, layers.at[0]), (viscosity_in, layers.at[1])))

    along_gx.greet(barrier)
    along_gy.greet(barrier)
    for group in [faces_in] + waves_in + [sides_in, tables_in, cells_in, kinds_in, layers_in]:
        start(group)

    def lanes(i):
        return slice(i * width, (i + 1) * width)

    def depths(i):
        return slice(i * half, (i + 1) * half)

    def cut_all(first, last, at):
        def part(where):
            return lambda halo, side: halo.at[side, :, where]
        return [(first.at[:, at(i)], last.at[:, at(i)], part(at(i))) for i in range(chunks)]

    def both_of(first, last):
        return [(f, l, lambda halo, side, i=i: halo.at[side, i]) for i, (f, l) in enumerate(zip(first, last))]

    p_z = Faces(along_gx, cut_all(*fz_p, lanes), hz_p, recv, 0)
    p_x = Faces(along_gy, cut_all(*fx_p, lanes), hx_p, recv, chunks)
    m_z = Faces(along_gx, cut_all(pm.at[0], pm.at[planes - 1], lanes), hz_m, recv, 2 * chunks)
    m_x = Faces(along_gy, cut_all(fx_m.at[0], fx_m.at[1], lanes), hx_m, recv, 3 * chunks)
    e_z = Faces(along_gx, cut_all(fz_e.at[0], fz_e.at[1], depths), hz_e, recv, 4 * chunks)
    e_x = Faces(along_gy, cut_all(fx_e.at[0], fx_e.at[1], depths), hx_e, recv, 5 * chunks)
    uw_z = Faces(along_gx, both_of(
        (u_in.at[0], w_in.at[0]), (u_in.at[tile_rows - 1], w_in.at[tile_rows - 1])), hz_uw, recv, 6 * chunks)
    uw_x = Faces(along_gy, both_of(
        (u_in.at[:, 0, :], w_in.at[:, 0, :]),
        (u_in.at[:, tile_cols - 1, :], w_in.at[:, tile_cols - 1, :])), hx_uw, recv, 6 * chunks + 2)

    faces_in[1].wait()
    pl.semaphore_wait(barrier, along_gx.neighbours + along_gy.neighbours)
    for i in range(chunks):
        p_x.start(i)
        p_z.start(i)
    for item in (uw_x, uw_z):
        item.start(0)
        item.start(1)
    along_gx.open()
    for item in (p_z, p_x, m_z, m_x, uw_z, uw_x, e_z, e_x):
        item.clear()

    def wave(now, before, lap, z):
        return (2.0 * now - before + c[z] * lap + n[z] * (now * now - before * before)
                - 0.1 * a[z] * (now - before))

    def first(z, up, down):
        now = p[z]
        mid = wave(now, q[z], laplace(now, up, down), z)
        pm[z] = mid
        fx_m[0, pl.ds(z, 1), :] = mid[:1]
        fx_m[1, pl.ds(z, 1), :] = mid[-1:]

    for i, group in enumerate(waves_in):
        group[1].wait()
        low, high = i * step - 1, (i + 1) * step - 1
        if i == 0:
            first(0, None, p[1])
            low = 1
        if i == cuts - 1:
            high = planes - 1
        lax.fori_loop(low, high, lambda z, carry: (first(z, p[z - 1], p[z + 1]), carry)[1], 0, unroll=2)
        if i == cuts - 1:
            first(planes - 1, p[planes - 2], None)
        if i == 0:
            along_gx.near()
        if i == min(1, cuts - 1):
            along_gx.far()
        if i == cuts - 1:
            along_gx.close()
            along_gy.open()
    sides_in[1].wait()

    for i in range(chunks):
        at = lanes(i)
        p_x.wait(i)
        p_z.wait(i)
        top = c[0, :, at] * hz_p[0, :, at]
        bottom = c[planes - 1, :, at] * hz_p[1, :, at]
        pm[0, :, at] = pm[0, :, at] + top
        pm[planes - 1, :, at] = pm[planes - 1, :, at] + bottom
        z = iota((planes, width), 0)
        for side, row in ((0, 0), (1, rows - 1)):
            extra = sides[side, :, at] * hx_p[side, :, at]
            extra = extra + jnp.where(z == 0, top[row:row + 1], 0.0)
            extra = extra + jnp.where(z == planes - 1, bottom[row:row + 1], 0.0)
            mid = fx_m[side, :, at] + extra
            fx_m[side, :, at] = mid
            pm[:, row, at] = mid
        m_x.start(i)
        m_z.start(i)
    along_gy.near()

    def second(z, up, down):
        now = pm[z]
        new = wave(now, p[z], laplace(now, up, down), z)
        pn[z] = new
        fx_n[0, pl.ds(z, 1), :] = new[:1]
        fx_n[1, pl.ds(z, 1), :] = new[-1:]
        return 0.1 * a[z] * (now * now + new * new) * lax.rsqrt(c[z])

    def pair_at(i):
        return pl.ds(pl.multiple_of(i * rows, rows), rows)

    paired[pair_at(0), :] = second(0, None, pm[1]) + second(1, pm[0], pm[2])
    last = planes // 2 - 1

    def two(i, carry):
        z = 2 * i
        paired[pair_at(i), :] = second(z, pm[z - 1], pm[z + 1]) + second(z + 1, pm[z], pm[z + 2])
        return carry

    middle = last // 2 + 1
    lax.fori_loop(1, middle, two, 0)
    along_gy.far()
    lax.fori_loop(middle, last, two, 0)
    paired[pair_at(last), :] = second(planes - 2, pm[planes - 3], pm[planes - 1]) + second(
        planes - 1, pm[planes - 2], None)
    gain[...] = 0.1 * sides[2:4] * lax.rsqrt(sides[0:2])

    tables_in[1].wait()
    lines_x, lines_z = own.shape
    count = lines_z * rows
    total = count + 2 * planes
    padded = -(-total // 128) * 128

    def line_of(column):
        beyond = column - count
        side = jnp.where(beyond >= planes, 1, 0)
        x = jnp.where(column < count, lax.rem(column, rows) // 2, side * (lines_x - 1))
        z = jnp.where(column < count, column // rows, (beyond - side * planes) // 2)
        return z, x

    def along_lanes(table):
        z_of, x_of = line_of(iota((lines_x, padded), 1))
        here = x_of == iota((lines_x, padded), 0)
        result = jnp.zeros((lines_x, padded), F32)
        for z in range(lines_z):
            result = result + jnp.where(here & (z_of == z), table[:, z:z + 1], 0.0)
        return jnp.sum(result, axis=0, keepdims=True)

    owners = own[...].astype(F32)
    owner_lane = along_lanes(owners)
    owner_row = jnp.transpose(jnp.broadcast_to(owner_lane, (128, padded)))[:count, :1]
    owner_lane = owner_lane[:, :total]
    place_lane = along_lanes(slot[...].astype(F32))[:, :total]
    z_of, x_of = line_of(iota((count, total), 1))
    earlier = iota((count, total), 0) // 2 < z_of * lines_x + x_of
    rank = 0.5 * jnp.sum(
        jnp.where((owner_row == owner_lane) & earlier, 1.0, 0.0), axis=0, keepdims=True)
    target = owner_lane * float(slots) + rank
    match = iota((blocks * slots, total), 0).astype(F32) == target
    column = iota((blocks * slots, total), 1)
    counted = (lax.rem(column, 2) == 0) & (column < count)
    places = jnp.sum(jnp.where(match & counted, place_lane + 1.0, 0.0), axis=1, keepdims=True)
    aligned = lax.rem(iota((blocks * slots, 128), 0), slots) == lax.rem(iota((blocks * slots, 128), 1), slots)
    places = jnp.where(aligned, places, 0.0).reshape(blocks, slots, 128)
    places = jnp.sum(places, axis=1, keepdims=True)
    match = jnp.where(match, 1.0, 0.0).astype(BF16)

    used = [pl.ds(0, capacity + 1)] + [pl.ds(0, capacity)] * (chunks - 1)
    others = pl.ds(0, blocks - 1)

    def line_copy(i, source, target_ref, x, y):
        return pltpu.make_async_remote_copy(
            src_ref=source, dst_ref=target_ref, send_sem=line_send.at[i], recv_sem=line_recv.at[i],
            device_id={"gx": x, "gy": y}, device_id_type=MESH)

    def turn(index, by, size):
        moved = index + by
        return jnp.where(moved >= size, moved - size, moved)

    far_first = sorted(range(gy), key=lambda by: -min(by, gy - by))
    xs, ys = [turn(me_x, by, gx) for by in range(gx)], [turn(me_y, by, gy) for by in range(gy)]

    def start_lines(i):
        def send(x, y):
            other = x * gy + y
            line_copy(i, packed.at[i, other, used[i]], got.at[i, me, used[i]], x, y).start()

        if blocks <= 32:
            for by in far_first:
                for ax in range(gx):
                    if by or ax:
                        send(xs[ax], ys[by])
        else:
            def one(d, carry):
                other = lax.rem(me + d, blocks)
                send(other // gy, lax.rem(other, gy))
                return carry

            lax.fori_loop(1, blocks, one, 0)
        got[i, me] = packed[i, me]

    all_lines = [line_copy(
        i, packed.at[i, others, used[i]], got.at[i, others, used[i]], me_x, me_y) for i in range(chunks)]

    lanes_two = jnp.where(iota((width, half), 0) // 2 == iota((width, half), 1), 0.125, 0.0).astype(BF16)
    for i in range(chunks):
        at = lanes(i)
        m_x.wait(i)
        m_z.wait(i)
        for side, z, pair in ((0, 0, 0), (1, planes - 1, last)):
            old = pn[z, :, at]
            extra = c[z, :, at] * hz_m[side, :, at]
            new = old + extra
            pn[z, :, at] = new
            fx_n[0, z:z + 1, at] = new[:1]
            fx_n[1, z:z + 1, at] = new[-1:]
            where = slice(pair * rows, (pair + 1) * rows)
            paired[where, at] = paired[where, at] + (
                0.1 * a[z, :, at] * lax.rsqrt(c[z, :, at]) * (extra * (2.0 * old + extra)))
        for side in range(2):
            old = fx_n[side, :, at]
            extra = sides[side, :, at] * hx_m[side, :, at]
            fx_n[side, :, at] = old + extra
            paired[count + side * planes:count + (side + 1) * planes, at] = (
                gain[side, :, at] * (extra * (2.0 * old + extra)))
        high, low = split(paired[:, at])
        coarse = dot(high, lanes_two) + dot(low, lanes_two)
        high, low = split(coarse)
        coarse = (dot(match, high) + dot(match, low)).reshape(blocks, slots, half)
        if i == 0:
            coarse = jnp.where(iota(coarse.shape, 1) == capacity, places, coarse)
            along_gy.close()
        packed[i] = coarse
        start_lines(i)

    for side, row in ((0, 0), (1, rows - 1)):
        pn[:, row, :] = fx_n[side]

    for group in (cells_in, kinds_in, layers_in):
        group[1].wait()
    for item in (uw_z, uw_x):
        item.wait(0)
        item.wait(1)

    def elastic(z, u_up, u_down, w_up, w_down):
        now, before, kind = u[z], w[z], k[z]
        lap_u = laplace(now, u_up, u_down, hx_uw[0, 0, pl.ds(z, 1), :], hx_uw[1, 0, pl.ds(z, 1), :])
        lap_w = laplace(before, w_up, w_down, hx_uw[0, 1, pl.ds(z, 1), :], hx_uw[1, 1, pl.ds(z, 1), :])
        shear, viscosity = jnp.zeros(now.shape, F32), jnp.zeros(now.shape, F32)
        for i in range(kinds):
            shear = jnp.where(kind == i, layers[0, i], shear)
            viscosity = jnp.where(kind == i, layers[1, i], viscosity)
        mid = 2.0 * now - before + shear * lap_u + viscosity * (lap_u - lap_w)
        um[z] = mid
        fx_e[0, pl.ds(z, 1), :] = mid[:1]
        fx_e[1, pl.ds(z, 1), :] = mid[-1:]
        rest[z] = now + viscosity * lap_u
        both[z] = shear + viscosity

    elastic(0, hz_uw[0, 0], u[1], hz_uw[0, 1], w[1])
    elastic(tile_rows - 1, u[tile_rows - 2], hz_uw[1, 0], w[tile_rows - 2], hz_uw[1, 1])
    lax.fori_loop(1, tile_rows - 1, lambda z, carry: (
        elastic(z, u[z - 1], u[z + 1], w[z - 1], w[z + 1]), carry)[1], 0)

    cells = tile_rows * tile_cols

    def landings():
        spread = -(-blocks * slots // 128)
        sources = jnp.concatenate([got[0, :, capacity, :]] * spread, axis=1)[:, :blocks * slots]
        mine = iota((blocks, blocks * slots), 1) // slots == iota((blocks, blocks * slots), 0)
        spots = jnp.sum(jnp.where(mine, sources, 0.0), axis=0, keepdims=True) - 1.0

        def landing_of(cell):
            return jnp.where(cell.astype(F32) == spots, 1.0, 0.0).astype(BF16)

        landing = landing_of(iota((cells, blocks * slots), 0))
        edges = 2 * tile_cols + 2 * tile_rows
        edge = iota((edges, blocks * slots), 0)
        beyond = edge - 2 * tile_cols
        edge_landing = landing_of(jnp.where(
            edge < tile_cols, edge, jnp.where(
                edge < 2 * tile_cols, edge + (cells - 2 * tile_cols), jnp.where(
                    beyond < tile_rows, beyond * tile_cols, (beyond - tile_rows) * tile_cols + tile_cols - 1))))
        real = lax.rem(iota((blocks * slots, half), 0), slots) < capacity
        return landing, edge_landing, real

    chunk = 4 if tile_rows % 4 == 0 else 1
    for i in range(chunks):
        at = depths(i)
        all_lines[i].wait_recv()
        if i == 0:
            landing, edge_landing, real = landings()
        lines = jnp.where(real, got[i].reshape(blocks * slots, half), 0.0)
        parts = jnp.concatenate(split(lines), axis=1)

        def sums(where):
            result = dot(where, parts)
            return result[:, :half] + result[:, half:]

        edge_force = 0.25 * sums(edge_landing)
        for side, z in ((0, 0), (1, tile_rows - 1)):
            fz_e[side, :, at] = um[z, :, at] + edge_force[side * tile_cols:(side + 1) * tile_cols]
            here = 2 * tile_cols + side * tile_rows
            fx_e[side, :, at] = fx_e[side, :, at] + edge_force[here:here + tile_rows]
        e_x.start(i)
        e_z.start(i)
        for r in range(0, tile_rows, chunk):
            force = sums(landing[r * tile_cols:(r + chunk) * tile_cols]).reshape(chunk, tile_cols, half)
            tf[r:r + chunk, :, at] = force
            um[r:r + chunk, :, at] = um[r:r + chunk, :, at] + 0.25 * force

    def final(z, up, down):
        now = um[z]
        un[z] = 2.0 * now - rest[z] + both[z] * laplace(now, up, down) + 0.25 * tf[z]

    final(0, None, um[1])
    final(tile_rows - 1, um[tile_rows - 2], None)
    lax.fori_loop(1, tile_rows - 1, lambda z, carry: (final(z, um[z - 1], um[z + 1]), carry)[1], 0, unroll=2)

    for item in all_lines:
        item.wait_send()
    for i in range(chunks):
        e_z.wait(i)
        e_x.wait(i)
    hz_out[...] = hz_e[...]
    hx_out[...] = hx_e[...]
    along_gx.wait_sent(paired, 2 * rows + 3 * tile_cols * tile_depth // lateral)
    along_gy.wait_sent(paired, 2 * planes + 3 * tile_rows * tile_depth // lateral)


def finish(pm, pn, tf, um, partial, both, hz, hx, pm_out, pn_out, tf_out, um_out, un_out, un, sems):
    copies = [pltpu.make_async_copy(s, d, sems.at[i]) for i, (s, d) in enumerate(
        ((pm, pm_out), (pn, pn_out), (tf, tf_out), (um, um_out)))]
    for copy in copies:
        copy.start()
    tile_rows, tile_cols, _ = um.shape

    def final(z, carry):
        scale = both[z]
        row = iota(scale.shape, 0)
        extra = jnp.where(row == 0, hx[0, pl.ds(z, 1), :], 0.0) + jnp.where(
            row == tile_cols - 1, hx[1, pl.ds(z, 1), :], 0.0)
        un[z] = partial[z] + scale * extra
        return carry

    lax.fori_loop(0, tile_rows, final, 0)
    for side, z in ((0, 0), (1, tile_rows - 1)):
        un[z] = un[z] + both[z] * hz[side]
    copies.append(pltpu.make_async_copy(un, un_out, sems.at[4]))
    copies[4].start()
    for copy in copies:
        copy.wait()


def local(pressure, pressure_prev, courant, nonlinearity, absorption, own_map, slot_table,
          displacement, displacement_prev, layer_labels, shear_table, viscosity_table):
    planes, rows, lateral = pressure.shape
    tile = displacement.shape
    blocks = lax.axis_size("gx") * lax.axis_size("gy")
    capacity = max(2, own_map.shape[0] * own_map.shape[1] // blocks)
    slots = -(-(capacity + 1) // 8) * 8
    width = 256
    chunks = lateral // width
    hbm = pl.BlockSpec(memory_space=pltpu.HBM)
    vmem = pl.BlockSpec(memory_space=pltpu.VMEM)
    wave, cell = pltpu.VMEM(pressure.shape, F32), pltpu.VMEM(tile, F32)

    def along_z(shape):
        return pltpu.VMEM((2,) + shape[1:], F32)

    def along_x(shape):
        return pltpu.VMEM((2, shape[0], shape[2]), F32)

    dma, regular = pltpu.SemaphoreType.DMA, pltpu.SemaphoreType.REGULAR
    kinds = shear_table.shape[0]
    wave_z, wave_x, cell_z, cell_x = along_z(pressure.shape), along_x(pressure.shape), along_z(tile), along_x(tile)
    lines = pltpu.VMEM((chunks, blocks, slots, width // 2), F32)
    waves = [jax.ShapeDtypeStruct(pressure.shape, F32)] * 2
    cells = [jax.ShapeDtypeStruct(tile, F32)]
    parts = pl.pallas_call(
        functools.partial(kernel, capacity, slots, width),
        out_shape=[wave] * 2 + [cell] * 4 + [cell_z, cell_x],
        in_specs=[hbm] * 12,
        out_specs=[vmem] * 8,
        scratch_shapes=[
            pltpu.VMEM((5,) + pressure.shape, F32), pltpu.VMEM((2,) + tile, F32), pltpu.VMEM(tile, jnp.int32),
            pltpu.VMEM((2,) + own_map.shape[::-1], jnp.int32), pltpu.SMEM((2, kinds), F32), dma((9,)),
            pltpu.VMEM((2 * (planes + rows), lateral), F32), pltpu.VMEM((4, planes, lateral), F32),
            wave_x, wave_x, cell_z, cell_x,
            wave_z, wave_x, wave_z, wave_x,
            pltpu.VMEM((2, 2) + tile[1:], F32), pltpu.VMEM((2, 2, tile[0], tile[2]), F32), cell_z, cell_x,
            cell, pltpu.VMEM((planes // 2 * rows + 2 * planes, lateral), F32), wave_x, lines, lines,
            dma((2,)), dma((2,)), dma((6 * chunks + 4,)), dma((chunks,)), dma((chunks,)), regular((2,)), regular((2,))],
        compiler_params=pltpu.CompilerParams(
            collective_id=0, has_side_effects=True, vmem_limit_bytes=58 * 1024 * 1024),
    )(pressure, pressure_prev, courant, nonlinearity, absorption, own_map.T, slot_table.T,
      displacement, displacement_prev, layer_labels, shear_table, viscosity_table)
    return pl.pallas_call(
        finish,
        out_shape=waves + cells * 3,
        in_specs=[vmem] * 8,
        out_specs=[hbm] * 5,
        scratch_shapes=[cell, dma((5,))],
        compiler_params=pltpu.CompilerParams(vmem_limit_bytes=40 * 1024 * 1024),
    )(*parts)


def solution(mesh):
    field = P(("group", "gx"), "gy", None)
    table = P(("group", "gx"), "gy")
    return jax.shard_map(
        local,
        mesh=mesh,
        in_specs=(field,) * 5 + (table,) * 2 + (field,) * 3 + (P("group"),) * 2,
        out_specs=(field,) * 5,
        check_vma=False,
    )
```

```python
import functools

import jax
import jax.numpy as jnp
from jax import lax
from jax.experimental import pallas as pl
from jax.experimental.pallas import tpu as pltpu
from jax.sharding import PartitionSpec as P

MESH = pl.DeviceIdType.MESH
F32 = jnp.float32
BF16 = jnp.bfloat16


def iota(shape, dim):
    return lax.broadcasted_iota(jnp.int32, shape, dim)


def split(x):
    high = x.astype(BF16)
    low = (x - high.astype(F32)).astype(BF16)
    return high, low


def dot(a, b):
    return jnp.dot(a, b, preferred_element_type=F32)


def laplace(centre, up, down, left=0.0, right=0.0):
    rows, lanes = centre.shape
    row, lane = iota(centre.shape, 0), iota(centre.shape, 1)
    xm = jnp.where(row == 0, left, pltpu.roll(centre, 1, 0))
    xp = jnp.where(row == rows - 1, right, pltpu.roll(centre, rows - 1, 0))
    ym = jnp.where(lane == 0, 0.0, pltpu.roll(centre, 1, 1))
    yp = jnp.where(lane == lanes - 1, 0.0, pltpu.roll(centre, lanes - 1, 1))
    if up is None:
        beside = down
    elif down is None:
        beside = up
    else:
        beside = up + down
    return (beside + (xm + xp)) + ((ym + yp) - 6.0 * centre)


class Faces:
    def __init__(self, line, pieces, halo, recv, base, together=False):
        self.line, self.halo = line, halo
        self.up, self.down, self.one, self.two = [], [], [], []
        for i, (first, last, part) in enumerate(pieces):
            arrived = recv.at[base if together else base + i]
            self.up.append(line.copy(last, part(halo, 0), arrived, True))
            self.down.append(line.copy(first, part(halo, 1), arrived, False))
        parts = [lambda halo, side: halo.at[side]] if together else [part for _, _, part in pieces]
        for i, part in enumerate(parts):
            arrived = recv.at[base + i]
            self.one.append(line.copy(part(halo, 0), part(halo, 0), arrived, True))
            self.two.append(line.copy(part(halo, slice(None)), part(halo, slice(None)), arrived, True))

    def clear(self):
        @pl.when(jnp.logical_not(self.line.has_prev))
        def _():
            self.halo[0] = jnp.zeros(self.halo.shape[1:], F32)

        @pl.when(jnp.logical_not(self.line.has_next))
        def _():
            self.halo[1] = jnp.zeros(self.halo.shape[1:], F32)

    def start(self, i=0):
        pl.when(self.line.has_next)(self.up[i].start)
        pl.when(self.line.has_prev)(self.down[i].start)

    def wait(self, i=0):
        pl.when(self.line.inside)(self.two[i].wait_recv)
        pl.when(self.line.at_end)(self.one[i].wait_recv)


class Line:
    def __init__(self, axis, sent, token):
        size, self.index = lax.axis_size(axis), lax.axis_index(axis)
        index = self.index
        self.size, self.axis, self.sent, self.token = size, axis, sent, token
        self.next = jnp.where(index == size - 1, 0, index + 1)
        self.prev = jnp.where(index == 0, size - 1, index - 1)
        self.has_next, self.has_prev = index < size - 1, index > 0
        self.inside = self.has_next & self.has_prev
        self.at_end = (index == 0) | (index == size - 1)
        self.low = index < size // 2
        self.neighbours = jnp.where(index < size - 1, 1, 0) + jnp.where(index > 0, 1, 0)

    def copy(self, source, target, arrived, up):
        return pltpu.make_async_remote_copy(
            src_ref=source, dst_ref=target, send_sem=self.sent.at[0 if up else 1], recv_sem=arrived,
            device_id={self.axis: self.next if up else self.prev}, device_id_type=MESH)

    def greet(self, barrier):
        for here, other in ((self.has_next, self.next), (self.has_prev, self.prev)):
            @pl.when(here)
            def _():
                pl.semaphore_signal(barrier, inc=1, device_id={self.axis: other}, device_id_type=MESH)

    def tell_next(self):
        pl.semaphore_signal(self.token.at[0], inc=1, device_id={self.axis: self.next}, device_id_type=MESH)

    def tell_prev(self):
        pl.semaphore_signal(self.token.at[1], inc=1, device_id={self.axis: self.prev}, device_id_type=MESH)

    def open(self):
        pl.when(self.index == 0)(self.tell_next)
        pl.when(self.index == self.size - 1)(self.tell_prev)

    def pass_up(self, where):
        @pl.when(where & self.inside)
        def _():
            pl.semaphore_wait(self.token.at[0], 1)
            self.tell_next()

    def pass_down(self, where):
        @pl.when(where & self.inside)
        def _():
            pl.semaphore_wait(self.token.at[1], 1)
            self.tell_prev()

    def near(self):
        self.pass_up(self.low)
        self.pass_down(jnp.logical_not(self.low))

    def far(self):
        self.pass_up(jnp.logical_not(self.low))
        self.pass_down(self.low)

    def close(self):
        @pl.when(self.index == 0)
        def _():
            pl.semaphore_wait(self.token.at[1], 1)

        @pl.when(self.index == self.size - 1)
        def _():
            pl.semaphore_wait(self.token.at[0], 1)

    def wait_sent(self, ref, size):
        whole = ref.at[0:size]
        pl.when(self.has_next)(self.copy(whole, whole, self.sent.at[0], True).wait_send)
        pl.when(self.has_prev)(self.copy(whole, whole, self.sent.at[0], False).wait_send)


def kernel(
    capacity, slots, width,
    p_in, q_in, c_in, n_in, a_in, own_in, slot_in, u_in, w_in, k_in, shear_in, viscosity_in,
    pm, pn, tf, um, un, both, hz_out, hx_out,
    fields, now_before, k, tables, layers, load,
    faces_p, sides, fx_m, fx_n, fz_e, fx_e,
    hz_p, hx_p, hz_m, hx_m, hz_uw, hx_uw, hz_e, hx_e,
    rest, paired, gain, packed, got,
    sent_z, sent_x, recv, line_send, line_recv, token_z, token_x,
):
    _, planes, rows, lateral = fields.shape
    _, tile_rows, tile_cols, tile_depth = now_before.shape
    kinds = layers.shape[1]
    p, q, c, n, a = (fields.at[i] for i in range(5))
    u, w = now_before.at[0], now_before.at[1]
    own, slot = tables.at[0], tables.at[1]
    fx_p = [faces_p.at[i * planes:(i + 1) * planes] for i in range(2)]
    fz_p = [faces_p.at[2 * planes + i * rows:2 * planes + (i + 1) * rows] for i in range(2)]
    fx_c, fx_a = sides.at[0:2], sides.at[2:4]
    half = width // 2
    chunks = lateral // width
    gx, gy = lax.axis_size("gx"), lax.axis_size("gy")
    blocks = gx * gy
    me_x, me_y = lax.axis_index("gx"), lax.axis_index("gy")
    me = me_x * gy + me_y
    along_gx, along_gy = Line("gx", sent_z, token_z), Line("gy", sent_x, token_x)

    barrier = pltpu.get_barrier_semaphore()
    cuts = 3 if planes % 3 == 0 else 1
    step = planes // cuts

    def loads(at, total, pairs):
        copies = [pltpu.make_async_copy(s, d, load.at[at]) for s, d in pairs]
        return copies, pltpu.make_async_copy(total, total, load.at[at])

    def start(group):
        for copy in group[0]:
            copy.start()

    faces_in = loads(0, faces_p, (
        (p_in.at[:, 0, :], fx_p[0]), (p_in.at[:, rows - 1, :], fx_p[1]),
        (p_in.at[0], fz_p[0]), (p_in.at[planes - 1], fz_p[1])))
    waves_in = []
    for i in range(cuts):
        part = pl.ds(i * step, step)
        waves_in.append(loads(6 + i, fields.at[:, part], [
            (s.at[part], fields.at[j, part]) for j, s in enumerate((p_in, q_in, c_in, n_in, a_in))]))
    tables_in = loads(1, tables, ((own_in, own), (slot_in, slot)))
    sides_in = loads(2, sides, (
        (c_in.at[:, 0, :], sides.at[0]), (c_in.at[:, rows - 1, :], sides.at[1]),
        (a_in.at[:, 0, :], sides.at[2]), (a_in.at[:, rows - 1, :], sides.at[3])))
    cells_in = loads(3, now_before, ((u_in, u), (w_in, w)))
    kinds_in = loads(4, k, ((k_in, k),))
    layers_in = loads(5, layers, ((shear_in, layers.at[0]), (viscosity_in, layers.at[1])))

    along_gx.greet(barrier)
    along_gy.greet(barrier)
    for group in [faces_in] + waves_in + [sides_in, tables_in, cells_in, kinds_in, layers_in]:
        start(group)

    def lanes(i):
        return slice(i * width, (i + 1) * width)

    def depths(i):
        return slice(i * half, (i + 1) * half)

    def cut_all(first, last, at):
        def part(where):
            return lambda halo, side: halo.at[side, :, where]
        return [(first.at[:, at(i)], last.at[:, at(i)], part(at(i))) for i in range(chunks)]

    def both_of(first, last):
        return [(f, l, lambda halo, side, i=i: halo.at[side, i]) for i, (f, l) in enumerate(zip(first, last))]

    p_z = Faces(along_gx, cut_all(*fz_p, lanes), hz_p, recv, 0)
    p_x = Faces(along_gy, cut_all(*fx_p, lanes), hx_p, recv, chunks)
    m_z = Faces(along_gx, cut_all(pm.at[0], pm.at[planes - 1], lanes), hz_m, recv, 2 * chunks)
    m_x = Faces(along_gy, cut_all(fx_m.at[0], fx_m.at[1], lanes), hx_m, recv, 3 * chunks)
    at = 4 * chunks
    e_z = Faces(along_gx, cut_all(fz_e.at[0], fz_e.at[1], depths), hz_e, recv, at, True)
    e_x = Faces(along_gy, cut_all(fx_e.at[0], fx_e.at[1], depths), hx_e, recv, at + 1, True)
    uw_z = Faces(along_gx, both_of(
        (u_in.at[0], w_in.at[0]), (u_in.at[tile_rows - 1], w_in.at[tile_rows - 1])), hz_uw, recv, at + 2, True)
    uw_x = Faces(along_gy, both_of(
        (u_in.at[:, 0, :], w_in.at[:, 0, :]),
        (u_in.at[:, tile_cols - 1, :], w_in.at[:, tile_cols - 1, :])), hx_uw, recv, at + 3, True)

    faces_in[1].wait()
    pl.semaphore_wait(barrier, along_gx.neighbours + along_gy.neighbours)
    for i in range(chunks):
        p_x.start(i)
        p_z.start(i)
    along_gx.open()
    for item in (p_z, p_x, m_z, m_x, uw_z, uw_x, e_z, e_x):
        item.clear()

    def wave(now, before, lap, z):
        return (2.0 * now - before + c[z] * lap + n[z] * (now * now - before * before)
                - 0.1 * a[z] * (now - before))

    def first(z, up, down):
        now = p[z]
        mid = wave(now, q[z], laplace(now, up, down), z)
        pm[z] = mid
        fx_m[0, pl.ds(z, 1), :] = mid[:1]
        fx_m[1, pl.ds(z, 1), :] = mid[-1:]

    for i, group in enumerate(waves_in):
        group[1].wait()
        low, high = i * step - 1, (i + 1) * step - 1
        if i == 0:
            first(0, None, p[1])
            low = 1
        if i == cuts - 1:
            high = planes - 1
        lax.fori_loop(low, high, lambda z, carry: (first(z, p[z - 1], p[z + 1]), carry)[1], 0, unroll=2)
        if i == cuts - 1:
            first(planes - 1, p[planes - 2], None)
        if i == 0:
            along_gx.near()
        if i == min(1, cuts - 1):
            along_gx.far()
        if i == cuts - 1:
            along_gx.close()
            along_gy.open()
    sides_in[1].wait()

    tables_in[1].wait()
    lines_x, lines_z = own.shape
    count = lines_z * rows
    total = count + 2 * planes
    padded = -(-total // 128) * 128

    def line_of(column):
        beyond = column - count
        side = jnp.where(beyond >= planes, 1, 0)
        x = jnp.where(column < count, lax.rem(column, rows) // 2, side * (lines_x - 1))
        z = jnp.where(column < count, column // rows, (beyond - side * planes) // 2)
        return z, x

    def along_lanes(table):
        z_of, x_of = line_of(iota((lines_x, padded), 1))
        here = x_of == iota((lines_x, padded), 0)
        result = jnp.zeros((lines_x, padded), F32)
        for z in range(lines_z):
            result = result + jnp.where(here & (z_of == z), table[:, z:z + 1], 0.0)
        return jnp.sum(result, axis=0, keepdims=True)

    owners = own[...].astype(F32)
    owner_lane = along_lanes(owners)
    owner_row = jnp.transpose(jnp.broadcast_to(owner_lane, (128, padded)))[:count, :1]
    owner_lane = owner_lane[:, :total]
    place_lane = along_lanes(slot[...].astype(F32))[:, :total]
    z_of, x_of = line_of(iota((count, total), 1))
    earlier = iota((count, total), 0) // 2 < z_of * lines_x + x_of
    rank = 0.5 * jnp.sum(
        jnp.where((owner_row == owner_lane) & earlier, 1.0, 0.0), axis=0, keepdims=True)
    target = owner_lane * float(slots) + rank
    match = iota((blocks * slots, total), 0).astype(F32) == target
    column = iota((blocks * slots, total), 1)
    counted = (lax.rem(column, 2) == 0) & (column < count)
    places = jnp.sum(jnp.where(match & counted, place_lane + 1.0, 0.0), axis=1, keepdims=True)
    aligned = lax.rem(iota((blocks * slots, 128), 0), slots) == lax.rem(iota((blocks * slots, 128), 1), slots)
    places = jnp.where(aligned, places, 0.0).reshape(blocks, slots, 128)
    places = jnp.sum(places, axis=1, keepdims=True)
    match = jnp.where(match, 1.0, 0.0).astype(BF16)

    for i in range(chunks):
        at = lanes(i)
        p_x.wait(i)
        p_z.wait(i)
        top = c[0, :, at] * hz_p[0, :, at]
        bottom = c[planes - 1, :, at] * hz_p[1, :, at]
        pm[0, :, at] = pm[0, :, at] + top
        pm[planes - 1, :, at] = pm[planes - 1, :, at] + bottom
        z = iota((planes, width), 0)
        for side, row in ((0, 0), (1, rows - 1)):
            extra = sides[side, :, at] * hx_p[side, :, at]
            extra = extra + jnp.where(z == 0, top[row:row + 1], 0.0)
            extra = extra + jnp.where(z == planes - 1, bottom[row:row + 1], 0.0)
            mid = fx_m[side, :, at] + extra
            fx_m[side, :, at] = mid
            pm[:, row, at] = mid
        m_x.start(i)
        m_z.start(i)
    for item in (uw_x, uw_z):
        item.start(0)
        item.start(1)
    along_gy.near()

    def second(z, up, down):
        now = pm[z]
        new = wave(now, p[z], laplace(now, up, down), z)
        pn[z] = new
        fx_n[0, pl.ds(z, 1), :] = new[:1]
        fx_n[1, pl.ds(z, 1), :] = new[-1:]
        return 0.1 * a[z] * (now * now + new * new) * lax.rsqrt(c[z])

    def pair_at(i):
        return pl.ds(pl.multiple_of(i * rows, rows), rows)

    paired[pair_at(0), :] = second(0, None, pm[1]) + second(1, pm[0], pm[2])
    last = planes // 2 - 1

    def two(i, carry):
        z = 2 * i
        paired[pair_at(i), :] = second(z, pm[z - 1], pm[z + 1]) + second(z + 1, pm[z], pm[z + 2])
        return carry

    middle = last // 2 + 1
    lax.fori_loop(1, middle, two, 0)
    along_gy.far()
    lax.fori_loop(middle, last, two, 0)
    paired[pair_at(last), :] = second(planes - 2, pm[planes - 3], pm[planes - 1]) + second(
        planes - 1, pm[planes - 2], None)
    gain[...] = 0.1 * sides[2:4] * lax.rsqrt(sides[0:2])

    used = [pl.ds(0, capacity + 1)] + [pl.ds(0, capacity)] * (chunks - 1)
    others = pl.ds(0, blocks - 1)

    def line_copy(i, source, target_ref, x, y):
        return pltpu.make_async_remote_copy(
            src_ref=source, dst_ref=target_ref, send_sem=line_send.at[i], recv_sem=line_recv.at[i],
            device_id={"gx": x, "gy": y}, device_id_type=MESH)

    def turn(index, by, size):
        moved = index + by
        return jnp.where(moved >= size, moved - size, moved)

    far_first = sorted(range(gy), key=lambda by: -min(by, gy - by))
    xs, ys = [turn(me_x, by, gx) for by in range(gx)], [turn(me_y, by, gy) for by in range(gy)]

    def start_lines(i):
        def send(x, y):
            other = x * gy + y
            line_copy(i, packed.at[i, other, used[i]], got.at[i, me, used[i]], x, y).start()

        if blocks <= 32:
            for by in far_first:
                for ax in range(gx):
                    if by or ax:
                        send(xs[ax], ys[by])
        else:
            def one(d, carry):
                other = lax.rem(me + d, blocks)
                send(other // gy, lax.rem(other, gy))
                return carry

            lax.fori_loop(1, blocks, one, 0)
        got[i, me] = packed[i, me]

    all_lines = [line_copy(
        i, packed.at[i, others, used[i]], got.at[i, others, used[i]], me_x, me_y) for i in range(chunks)]

    lanes_two = jnp.where(iota((width, half), 0) // 2 == iota((width, half), 1), 0.125, 0.0).astype(BF16)
    for i in range(chunks):
        at = lanes(i)
        m_x.wait(i)
        m_z.wait(i)
        for side, z, pair in ((0, 0, 0), (1, planes - 1, last)):
            old = pn[z, :, at]
            extra = c[z, :, at] * hz_m[side, :, at]
            new = old + extra
            pn[z, :, at] = new
            fx_n[0, z:z + 1, at] = new[:1]
            fx_n[1, z:z + 1, at] = new[-1:]
            where = slice(pair * rows, (pair + 1) * rows)
            paired[where, at] = paired[where, at] + (
                0.1 * a[z, :, at] * lax.rsqrt(c[z, :, at]) * (extra * (2.0 * old + extra)))
        for side in range(2):
            old = fx_n[side, :, at]
            extra = sides[side, :, at] * hx_m[side, :, at]
            fx_n[side, :, at] = old + extra
            paired[count + side * planes:count + (side + 1) * planes, at] = (
                gain[side, :, at] * (extra * (2.0 * old + extra)))
        high, low = split(paired[:, at])
        coarse = dot(high, lanes_two) + dot(low, lanes_two)
        high, low = split(coarse)
        coarse = (dot(match, high) + dot(match, low)).reshape(blocks, slots, half)
        if i == 0:
            coarse = jnp.where(iota(coarse.shape, 1) == capacity, places, coarse)
            along_gy.close()
        packed[i] = coarse
        start_lines(i)

    for side, row in ((0, 0), (1, rows - 1)):
        pn[:, row, :] = fx_n[side]

    for group in (cells_in, kinds_in, layers_in):
        group[1].wait()
    uw_z.wait()
    uw_x.wait()

    def elastic(z, u_up, u_down, w_up, w_down):
        now, before, kind = u[z], w[z], k[z]
        lap_u = laplace(now, u_up, u_down, hx_uw[0, 0, pl.ds(z, 1), :], hx_uw[1, 0, pl.ds(z, 1), :])
        lap_w = laplace(before, w_up, w_down, hx_uw[0, 1, pl.ds(z, 1), :], hx_uw[1, 1, pl.ds(z, 1), :])
        shear, viscosity = jnp.zeros(now.shape, F32), jnp.zeros(now.shape, F32)
        for i in range(kinds):
            shear = jnp.where(kind == i, layers[0, i], shear)
            viscosity = jnp.where(kind == i, layers[1, i], viscosity)
        mid = 2.0 * now - before + shear * lap_u + viscosity * (lap_u - lap_w)
        um[z] = mid
        fx_e[0, pl.ds(z, 1), :] = mid[:1]
        fx_e[1, pl.ds(z, 1), :] = mid[-1:]
        rest[z] = now + viscosity * lap_u
        both[z] = shear + viscosity

    elastic(0, hz_uw[0, 0], u[1], hz_uw[0, 1], w[1])
    elastic(tile_rows - 1, u[tile_rows - 2], hz_uw[1, 0], w[tile_rows - 2], hz_uw[1, 1])
    lax.fori_loop(1, tile_rows - 1, lambda z, carry: (
        elastic(z, u[z - 1], u[z + 1], w[z - 1], w[z + 1]), carry)[1], 0)

    cells = tile_rows * tile_cols

    def landings():
        spread = -(-blocks * slots // 128)
        sources = jnp.concatenate([got[0, :, capacity, :]] * spread, axis=1)[:, :blocks * slots]
        mine = iota((blocks, blocks * slots), 1) // slots == iota((blocks, blocks * slots), 0)
        spots = jnp.sum(jnp.where(mine, sources, 0.0), axis=0, keepdims=True) - 1.0

        def landing_of(cell):
            return jnp.where(cell.astype(F32) == spots, 1.0, 0.0).astype(BF16)

        landing = landing_of(iota((cells, blocks * slots), 0))
        edges = 2 * tile_cols + 2 * tile_rows
        edge = iota((edges, blocks * slots), 0)
        beyond = edge - 2 * tile_cols
        edge_landing = landing_of(jnp.where(
            edge < tile_cols, edge, jnp.where(
                edge < 2 * tile_cols, edge + (cells - 2 * tile_cols), jnp.where(
                    beyond < tile_rows, beyond * tile_cols, (beyond - tile_rows) * tile_cols + tile_cols - 1))))
        real = lax.rem(iota((blocks * slots, half), 0), slots) < capacity
        return landing, edge_landing, real

    chunk = 4 if tile_rows % 4 == 0 else 1
    for i in range(chunks):
        at = depths(i)
        all_lines[i].wait_recv()
        if i == 0:
            landing, edge_landing, real = landings()
        lines = jnp.where(real, got[i].reshape(blocks * slots, half), 0.0)
        parts = jnp.concatenate(split(lines), axis=1)

        def sums(where):
            result = dot(where, parts)
            return result[:, :half] + result[:, half:]

        edge_force = 0.25 * sums(edge_landing)
        for side, z in ((0, 0), (1, tile_rows - 1)):
            fz_e[side, :, at] = um[z, :, at] + edge_force[side * tile_cols:(side + 1) * tile_cols]
            here = 2 * tile_cols + side * tile_rows
            fx_e[side, :, at] = fx_e[side, :, at] + edge_force[here:here + tile_rows]
        e_x.start(i)
        e_z.start(i)
        for r in range(0, tile_rows, chunk):
            force = sums(landing[r * tile_cols:(r + chunk) * tile_cols]).reshape(chunk, tile_cols, half)
            tf[r:r + chunk, :, at] = force
            um[r:r + chunk, :, at] = um[r:r + chunk, :, at] + 0.25 * force

    def final(z, up, down):
        now = um[z]
        un[z] = 2.0 * now - rest[z] + both[z] * laplace(now, up, down) + 0.25 * tf[z]

    final(0, None, um[1])
    final(tile_rows - 1, um[tile_rows - 2], None)
    lax.fori_loop(1, tile_rows - 1, lambda z, carry: (final(z, um[z - 1], um[z + 1]), carry)[1], 0, unroll=2)

    for item in all_lines:
        item.wait_send()
    e_z.wait()
    e_x.wait()
    hz_out[...] = hz_e[...]
    hx_out[...] = hx_e[...]
    along_gx.wait_sent(paired, 2 * rows + 3 * tile_cols * tile_depth // lateral)
    along_gy.wait_sent(paired, 2 * planes + 3 * tile_rows * tile_depth // lateral)


def finish(pm, pn, tf, um, partial, both, hz, hx, pm_out, pn_out, tf_out, um_out, un_out, un, sems):
    copies = [pltpu.make_async_copy(s, d, sems.at[i]) for i, (s, d) in enumerate(
        ((pm, pm_out), (pn, pn_out), (tf, tf_out), (um, um_out)))]
    for copy in copies:
        copy.start()
    tile_rows, tile_cols, _ = um.shape

    def final(z, carry):
        scale = both[z]
        row = iota(scale.shape, 0)
        extra = jnp.where(row == 0, hx[0, pl.ds(z, 1), :], 0.0) + jnp.where(
            row == tile_cols - 1, hx[1, pl.ds(z, 1), :], 0.0)
        un[z] = partial[z] + scale * extra
        return carry

    lax.fori_loop(0, tile_rows, final, 0)
    for side, z in ((0, 0), (1, tile_rows - 1)):
        un[z] = un[z] + both[z] * hz[side]
    copies.append(pltpu.make_async_copy(un, un_out, sems.at[4]))
    copies[4].start()
    for copy in copies:
        copy.wait()


def local(pressure, pressure_prev, courant, nonlinearity, absorption, own_map, slot_table,
          displacement, displacement_prev, layer_labels, shear_table, viscosity_table):
    planes, rows, lateral = pressure.shape
    tile = displacement.shape
    blocks = lax.axis_size("gx") * lax.axis_size("gy")
    capacity = max(2, own_map.shape[0] * own_map.shape[1] // blocks)
    slots = -(-(capacity + 1) // 8) * 8
    width = 256
    chunks = lateral // width
    hbm = pl.BlockSpec(memory_space=pltpu.HBM)
    vmem = pl.BlockSpec(memory_space=pltpu.VMEM)
    wave, cell = pltpu.VMEM(pressure.shape, F32), pltpu.VMEM(tile, F32)

    def along_z(shape):
        return pltpu.VMEM((2,) + shape[1:], F32)

    def along_x(shape):
        return pltpu.VMEM((2, shape[0], shape[2]), F32)

    dma, regular = pltpu.SemaphoreType.DMA, pltpu.SemaphoreType.REGULAR
    kinds = shear_table.shape[0]
    wave_z, wave_x, cell_z, cell_x = along_z(pressure.shape), along_x(pressure.shape), along_z(tile), along_x(tile)
    lines = pltpu.VMEM((chunks, blocks, slots, width // 2), F32)
    waves = [jax.ShapeDtypeStruct(pressure.shape, F32)] * 2
    cells = [jax.ShapeDtypeStruct(tile, F32)]
    parts = pl.pallas_call(
        functools.partial(kernel, capacity, slots, width),
        out_shape=[wave] * 2 + [cell] * 4 + [cell_z, cell_x],
        in_specs=[hbm] * 12,
        out_specs=[vmem] * 8,
        scratch_shapes=[
            pltpu.VMEM((5,) + pressure.shape, F32), pltpu.VMEM((2,) + tile, F32), pltpu.VMEM(tile, jnp.int32),
            pltpu.VMEM((2,) + own_map.shape[::-1], jnp.int32), pltpu.SMEM((2, kinds), F32), dma((9,)),
            pltpu.VMEM((2 * (planes + rows), lateral), F32), pltpu.VMEM((4, planes, lateral), F32),
            wave_x, wave_x, cell_z, cell_x,
            wave_z, wave_x, wave_z, wave_x,
            pltpu.VMEM((2, 2) + tile[1:], F32), pltpu.VMEM((2, 2, tile[0], tile[2]), F32), cell_z, cell_x,
            cell, pltpu.VMEM((planes // 2 * rows + 2 * planes, lateral), F32), wave_x, lines, lines,
            dma((2,)), dma((2,)), dma((4 * chunks + 4,)), dma((chunks,)), dma((chunks,)), regular((2,)), regular((2,))],
        compiler_params=pltpu.CompilerParams(
            collective_id=0, has_side_effects=True, vmem_limit_bytes=58 * 1024 * 1024),
    )(pressure, pressure_prev, courant, nonlinearity, absorption, own_map.T, slot_table.T,
      displacement, displacement_prev, layer_labels, shear_table, viscosity_table)
    return pl.pallas_call(
        finish,
        out_shape=waves + cells * 3,
        in_specs=[vmem] * 8,
        out_specs=[hbm] * 5,
        scratch_shapes=[cell, dma((5,))],
        compiler_params=pltpu.CompilerParams(vmem_limit_bytes=40 * 1024 * 1024),
    )(*parts)


def solution(mesh):
    field = P(("group", "gx"), "gy", None)
    table = P(("group", "gx"), "gy")
    return jax.shard_map(
        local,
        mesh=mesh,
        in_specs=(field,) * 5 + (table,) * 2 + (field,) * 3 + (P("group"),) * 2,
        out_specs=(field,) * 5,
        check_vma=False,
    )
```

```python
import functools

import jax
import jax.numpy as jnp
from jax import lax
from jax.experimental import pallas as pl
from jax.experimental.pallas import tpu as pltpu
from jax.sharding import PartitionSpec as P

MESH = pl.DeviceIdType.MESH
F32 = jnp.float32
BF16 = jnp.bfloat16


def iota(shape, dim):
    return lax.broadcasted_iota(jnp.int32, shape, dim)


def split(x):
    high = x.astype(BF16)
    low = (x - high.astype(F32)).astype(BF16)
    return high, low


def dot(a, b):
    return jnp.dot(a, b, preferred_element_type=F32)


def laplace(centre, up, down, left=0.0, right=0.0):
    rows, lanes = centre.shape
    row, lane = iota(centre.shape, 0), iota(centre.shape, 1)
    xm = jnp.where(row == 0, left, pltpu.roll(centre, 1, 0))
    xp = jnp.where(row == rows - 1, right, pltpu.roll(centre, rows - 1, 0))
    ym = jnp.where(lane == 0, 0.0, pltpu.roll(centre, 1, 1))
    yp = jnp.where(lane == lanes - 1, 0.0, pltpu.roll(centre, lanes - 1, 1))
    if up is None:
        beside = down
    elif down is None:
        beside = up
    else:
        beside = up + down
    return (beside + (xm + xp)) + ((ym + yp) - 6.0 * centre)


class Faces:
    def __init__(self, line, pieces, halo, recv, base, together=False):
        self.line, self.halo = line, halo
        self.up, self.down, self.one, self.two = [], [], [], []
        for i, (first, last, part) in enumerate(pieces):
            arrived = recv.at[base if together else base + i]
            self.up.append(line.copy(last, part(halo, 0), arrived, True))
            self.down.append(line.copy(first, part(halo, 1), arrived, False))
        parts = [lambda halo, side: halo.at[side]] if together else [part for _, _, part in pieces]
        for i, part in enumerate(parts):
            arrived = recv.at[base + i]
            self.one.append(line.copy(part(halo, 0), part(halo, 0), arrived, True))
            self.two.append(line.copy(part(halo, slice(None)), part(halo, slice(None)), arrived, True))

    def clear(self):
        @pl.when(jnp.logical_not(self.line.has_prev))
        def _():
            self.halo[0] = jnp.zeros(self.halo.shape[1:], F32)

        @pl.when(jnp.logical_not(self.line.has_next))
        def _():
            self.halo[1] = jnp.zeros(self.halo.shape[1:], F32)

    def start(self, i=0):
        pl.when(self.line.has_next)(self.up[i].start)
        pl.when(self.line.has_prev)(self.down[i].start)

    def wait(self, i=0):
        pl.when(self.line.inside)(self.two[i].wait_recv)
        pl.when(self.line.at_end)(self.one[i].wait_recv)


class Line:
    def __init__(self, axis, sent, token):
        size, self.index = lax.axis_size(axis), lax.axis_index(axis)
        index = self.index
        self.size, self.axis, self.sent, self.token = size, axis, sent, token
        self.next = jnp.where(index == size - 1, 0, index + 1)
        self.prev = jnp.where(index == 0, size - 1, index - 1)
        self.has_next, self.has_prev = index < size - 1, index > 0
        self.inside = self.has_next & self.has_prev
        self.at_end = (index == 0) | (index == size - 1)
        self.low = index < size // 2
        self.neighbours = jnp.where(index < size - 1, 1, 0) + jnp.where(index > 0, 1, 0)

    def copy(self, source, target, arrived, up):
        return pltpu.make_async_remote_copy(
            src_ref=source, dst_ref=target, send_sem=self.sent.at[0 if up else 1], recv_sem=arrived,
            device_id={self.axis: self.next if up else self.prev}, device_id_type=MESH)

    def greet(self, barrier):
        for here, other in ((self.has_next, self.next), (self.has_prev, self.prev)):
            @pl.when(here)
            def _():
                pl.semaphore_signal(barrier, inc=1, device_id={self.axis: other}, device_id_type=MESH)

    def tell_next(self):
        pl.semaphore_signal(self.token.at[0], inc=1, device_id={self.axis: self.next}, device_id_type=MESH)

    def tell_prev(self):
        pl.semaphore_signal(self.token.at[1], inc=1, device_id={self.axis: self.prev}, device_id_type=MESH)

    def open(self):
        pl.when(self.index == 0)(self.tell_next)
        pl.when(self.index == self.size - 1)(self.tell_prev)

    def pass_up(self, where):
        @pl.when(where & self.inside)
        def _():
            pl.semaphore_wait(self.token.at[0], 1)
            self.tell_next()

    def pass_down(self, where):
        @pl.when(where & self.inside)
        def _():
            pl.semaphore_wait(self.token.at[1], 1)
            self.tell_prev()

    def near(self):
        self.pass_up(self.low)
        self.pass_down(jnp.logical_not(self.low))

    def far(self):
        self.pass_up(jnp.logical_not(self.low))
        self.pass_down(self.low)

    def close(self):
        @pl.when(self.index == 0)
        def _():
            pl.semaphore_wait(self.token.at[1], 1)

        @pl.when(self.index == self.size - 1)
        def _():
            pl.semaphore_wait(self.token.at[0], 1)

    def wait_sent(self, ref, size):
        whole = ref.at[0:size]
        pl.when(self.has_next)(self.copy(whole, whole, self.sent.at[0], True).wait_send)
        pl.when(self.has_prev)(self.copy(whole, whole, self.sent.at[0], False).wait_send)


def kernel(
    capacity, slots, width,
    p_in, q_in, c_in, n_in, a_in, own_in, slot_in, u_in, w_in, k_in, shear_in, viscosity_in,
    pm, pn, tf, um, un, both, hz_out, hx_out,
    fields, now_before, k, tables, layers, load,
    faces_p, sides, fx_m, fx_n, fz_e, fx_e,
    hz_p, hx_p, hz_m, hx_m, hz_uw, hx_uw, hz_e, hx_e,
    rest, paired, gain, packed, got,
    sent_z, sent_x, recv, line_send, line_recv, token_z, token_x,
):
    _, planes, rows, lateral = fields.shape
    _, tile_rows, tile_cols, tile_depth = now_before.shape
    kinds = layers.shape[1]
    p, q, c, n, a = (fields.at[i] for i in range(5))
    u, w = now_before.at[0], now_before.at[1]
    own, slot = tables.at[0], tables.at[1]
    fx_p = [faces_p.at[i * planes:(i + 1) * planes] for i in range(2)]
    fz_p = [faces_p.at[2 * planes + i * rows:2 * planes + (i + 1) * rows] for i in range(2)]
    fx_c, fx_a = sides.at[0:2], sides.at[2:4]
    half = width // 2
    chunks = lateral // width
    gx, gy = lax.axis_size("gx"), lax.axis_size("gy")
    blocks = gx * gy
    me_x, me_y = lax.axis_index("gx"), lax.axis_index("gy")
    me = me_x * gy + me_y
    along_gx, along_gy = Line("gx", sent_z, token_z), Line("gy", sent_x, token_x)

    barrier = pltpu.get_barrier_semaphore()
    cuts = 6 if planes % 6 == 0 else 1
    step = planes // cuts

    def loads(at, total, pairs):
        copies = [pltpu.make_async_copy(s, d, load.at[at]) for s, d in pairs]
        return copies, pltpu.make_async_copy(total, total, load.at[at])

    def start(group):
        for copy in group[0]:
            copy.start()

    faces_in = loads(0, faces_p, (
        (p_in.at[:, 0, :], fx_p[0]), (p_in.at[:, rows - 1, :], fx_p[1]),
        (p_in.at[0], fz_p[0]), (p_in.at[planes - 1], fz_p[1])))
    waves_in = []
    for i in range(cuts):
        part = pl.ds(i * step, step)
        waves_in.append(loads(6 + i, fields.at[:, part], [
            (s.at[part], fields.at[j, part]) for j, s in enumerate((p_in, q_in, c_in, n_in, a_in))]))
    tables_in = loads(1, tables, ((own_in, own), (slot_in, slot)))
    sides_in = loads(2, sides, (
        (c_in.at[:, 0, :], sides.at[0]), (c_in.at[:, rows - 1, :], sides.at[1]),
        (a_in.at[:, 0, :], sides.at[2]), (a_in.at[:, rows - 1, :], sides.at[3])))
    cells_in = loads(3, now_before, ((u_in, u), (w_in, w)))
    kinds_in = loads(4, k, ((k_in, k),))
    layers_in = loads(5, layers, ((shear_in, layers.at[0]), (viscosity_in, layers.at[1])))

    along_gx.greet(barrier)
    along_gy.greet(barrier)
    for group in [faces_in] + waves_in + [sides_in, tables_in, cells_in, kinds_in, layers_in]:
        start(group)

    def lanes(i):
        return slice(i * width, (i + 1) * width)

    def depths(i):
        return slice(i * half, (i + 1) * half)

    def cut_all(first, last, at):
        def part(where):
            return lambda halo, side: halo.at[side, :, where]
        return [(first.at[:, at(i)], last.at[:, at(i)], part(at(i))) for i in range(chunks)]

    def both_of(first, last):
        return [(f, l, lambda halo, side, i=i: halo.at[side, i]) for i, (f, l) in enumerate(zip(first, last))]

    p_z = Faces(along_gx, cut_all(*fz_p, lanes), hz_p, recv, 0)
    p_x = Faces(along_gy, cut_all(*fx_p, lanes), hx_p, recv, chunks)
    m_z = Faces(along_gx, cut_all(pm.at[0], pm.at[planes - 1], lanes), hz_m, recv, 2 * chunks)
    m_x = Faces(along_gy, cut_all(fx_m.at[0], fx_m.at[1], lanes), hx_m, recv, 3 * chunks)
    at = 4 * chunks
    e_z = Faces(along_gx, cut_all(fz_e.at[0], fz_e.at[1], depths), hz_e, recv, at, True)
    e_x = Faces(along_gy, cut_all(fx_e.at[0], fx_e.at[1], depths), hx_e, recv, at + 1, True)
    uw_z = Faces(along_gx, both_of(
        (u_in.at[0], w_in.at[0]), (u_in.at[tile_rows - 1], w_in.at[tile_rows - 1])), hz_uw, recv, at + 2, True)
    uw_x = Faces(along_gy, both_of(
        (u_in.at[:, 0, :], w_in.at[:, 0, :]),
        (u_in.at[:, tile_cols - 1, :], w_in.at[:, tile_cols - 1, :])), hx_uw, recv, at + 3, True)

    faces_in[1].wait()
    pl.semaphore_wait(barrier, along_gx.neighbours + along_gy.neighbours)
    for i in range(chunks):
        p_x.start(i)
        p_z.start(i)
    along_gx.open()
    for item in (p_z, p_x, m_z, m_x, uw_z, uw_x, e_z, e_x):
        item.clear()

    def wave(now, before, lap, z):
        return (2.0 * now - before + c[z] * lap + n[z] * (now * now - before * before)
                - 0.1 * a[z] * (now - before))

    def first(z, up, down):
        now = p[z]
        mid = wave(now, q[z], laplace(now, up, down), z)
        pm[z] = mid
        fx_m[0, pl.ds(z, 1), :] = mid[:1]
        fx_m[1, pl.ds(z, 1), :] = mid[-1:]

    for i, group in enumerate(waves_in):
        group[1].wait()
        low, high = i * step - 1, (i + 1) * step - 1
        if i == 0:
            first(0, None, p[1])
            low = 1
        if i == cuts - 1:
            high = planes - 1
        lax.fori_loop(low, high, lambda z, carry: (first(z, p[z - 1], p[z + 1]), carry)[1], 0, unroll=2)
        if i == cuts - 1:
            first(planes - 1, p[planes - 2], None)
        if i == (cuts + 2) // 3 - 1:
            along_gx.near()
        if i == max(2 * cuts // 3 - 1, 0):
            along_gx.far()
        if i == cuts - 1:
            along_gx.close()
            along_gy.open()
    sides_in[1].wait()

    tables_in[1].wait()
    lines_x, lines_z = own.shape
    count = lines_z * rows
    total = count + 2 * planes
    padded = -(-total // 128) * 128

    def line_of(column):
        beyond = column - count
        side = jnp.where(beyond >= planes, 1, 0)
        x = jnp.where(column < count, lax.rem(column, rows) // 2, side * (lines_x - 1))
        z = jnp.where(column < count, column // rows, (beyond - side * planes) // 2)
        return z, x

    def along_lanes(table):
        z_of, x_of = line_of(iota((lines_x, padded), 1))
        here = x_of == iota((lines_x, padded), 0)
        result = jnp.zeros((lines_x, padded), F32)
        for z in range(lines_z):
            result = result + jnp.where(here & (z_of == z), table[:, z:z + 1], 0.0)
        return jnp.sum(result, axis=0, keepdims=True)

    owners = own[...].astype(F32)
    owner_lane = along_lanes(owners)
    owner_row = jnp.transpose(jnp.broadcast_to(owner_lane, (128, padded)))[:count, :1]
    owner_lane = owner_lane[:, :total]
    place_lane = along_lanes(slot[...].astype(F32))[:, :total]
    z_of, x_of = line_of(iota((count, total), 1))
    earlier = iota((count, total), 0) // 2 < z_of * lines_x + x_of
    rank = 0.5 * jnp.sum(
        jnp.where((owner_row == owner_lane) & earlier, 1.0, 0.0), axis=0, keepdims=True)
    target = owner_lane * float(slots) + rank
    match = iota((blocks * slots, total), 0).astype(F32) == target
    column = iota((blocks * slots, total), 1)
    counted = (lax.rem(column, 2) == 0) & (column < count)
    places = jnp.sum(jnp.where(match & counted, place_lane + 1.0, 0.0), axis=1, keepdims=True)
    aligned = lax.rem(iota((blocks * slots, 128), 0), slots) == lax.rem(iota((blocks * slots, 128), 1), slots)
    places = jnp.where(aligned, places, 0.0).reshape(blocks, slots, 128)
    places = jnp.sum(places, axis=1, keepdims=True)
    match = jnp.where(match, 1.0, 0.0).astype(BF16)

    for i in range(chunks):
        at = lanes(i)
        p_x.wait(i)
        p_z.wait(i)
        top = c[0, :, at] * hz_p[0, :, at]
        bottom = c[planes - 1, :, at] * hz_p[1, :, at]
        pm[0, :, at] = pm[0, :, at] + top
        pm[planes - 1, :, at] = pm[planes - 1, :, at] + bottom
        z = iota((planes, width), 0)
        for side, row in ((0, 0), (1, rows - 1)):
            extra = sides[side, :, at] * hx_p[side, :, at]
            extra = extra + jnp.where(z == 0, top[row:row + 1], 0.0)
            extra = extra + jnp.where(z == planes - 1, bottom[row:row + 1], 0.0)
            mid = fx_m[side, :, at] + extra
            fx_m[side, :, at] = mid
            pm[:, row, at] = mid
        m_x.start(i)
        m_z.start(i)
    for item in (uw_x, uw_z):
        item.start(0)
        item.start(1)
    along_gy.near()

    def second(z, up, down):
        now = pm[z]
        new = wave(now, p[z], laplace(now, up, down), z)
        pn[z] = new
        fx_n[0, pl.ds(z, 1), :] = new[:1]
        fx_n[1, pl.ds(z, 1), :] = new[-1:]
        return 0.1 * a[z] * (now * now + new * new) * lax.rsqrt(c[z])

    def pair_at(i):
        return pl.ds(pl.multiple_of(i * rows, rows), rows)

    paired[pair_at(0), :] = second(0, None, pm[1]) + second(1, pm[0], pm[2])
    last = planes // 2 - 1

    def two(i, carry):
        z = 2 * i
        paired[pair_at(i), :] = second(z, pm[z - 1], pm[z + 1]) + second(z + 1, pm[z], pm[z + 2])
        return carry

    middle = last // 2 + 1
    lax.fori_loop(1, middle, two, 0)
    along_gy.far()
    lax.fori_loop(middle, last, two, 0)
    paired[pair_at(last), :] = second(planes - 2, pm[planes - 3], pm[planes - 1]) + second(
        planes - 1, pm[planes - 2], None)
    gain[...] = 0.1 * sides[2:4] * lax.rsqrt(sides[0:2])

    used = [pl.ds(0, capacity + 1)] + [pl.ds(0, capacity)] * (chunks - 1)
    others = pl.ds(0, blocks - 1)

    def line_copy(i, source, target_ref, x, y):
        return pltpu.make_async_remote_copy(
            src_ref=source, dst_ref=target_ref, send_sem=line_send.at[i], recv_sem=line_recv.at[i],
            device_id={"gx": x, "gy": y}, device_id_type=MESH)

    def far_first(index, size):
        def place(j):
            down, low = size - 1 - j, index < size // 2
            return jnp.where(low, jnp.where(down > index, down, down - 1), jnp.where(j < index, j, j + 1))

        return [place(j) for j in range(size - 1)] + [index]

    xs, ys = far_first(me_x, gx), far_first(me_y, gy)

    def start_lines(i):
        def send(x, y):
            other = x * gy + y
            line_copy(i, packed.at[i, other, used[i]], got.at[i, me, used[i]], x, y).start()

        if blocks <= 32:
            for y in ys:
                for x in xs:
                    if x is not me_x or y is not me_y:
                        send(x, y)
        else:
            def one(d, carry):
                other = lax.rem(me + d, blocks)
                send(other // gy, lax.rem(other, gy))
                return carry

            lax.fori_loop(1, blocks, one, 0)
        got[i, me] = packed[i, me]

    all_lines = [line_copy(
        i, packed.at[i, others, used[i]], got.at[i, others, used[i]], me_x, me_y) for i in range(chunks)]

    lanes_two = jnp.where(iota((width, half), 0) // 2 == iota((width, half), 1), 0.125, 0.0).astype(BF16)
    for i in range(chunks):
        at = lanes(i)
        m_x.wait(i)
        m_z.wait(i)
        for side, z, pair in ((0, 0, 0), (1, planes - 1, last)):
            old = pn[z, :, at]
            extra = c[z, :, at] * hz_m[side, :, at]
            new = old + extra
            pn[z, :, at] = new
            fx_n[0, z:z + 1, at] = new[:1]
            fx_n[1, z:z + 1, at] = new[-1:]
            where = slice(pair * rows, (pair + 1) * rows)
            paired[where, at] = paired[where, at] + (
                0.1 * a[z, :, at] * lax.rsqrt(c[z, :, at]) * (extra * (2.0 * old + extra)))
        for side in range(2):
            old = fx_n[side, :, at]
            extra = sides[side, :, at] * hx_m[side, :, at]
            fx_n[side, :, at] = old + extra
            paired[count + side * planes:count + (side + 1) * planes, at] = (
                gain[side, :, at] * (extra * (2.0 * old + extra)))
        high, low = split(paired[:, at])
        coarse = dot(high, lanes_two) + dot(low, lanes_two)
        high, low = split(coarse)
        coarse = (dot(match, high) + dot(match, low)).reshape(blocks, slots, half)
        if i == 0:
            coarse = jnp.where(iota(coarse.shape, 1) == capacity, places, coarse)
            along_gy.close()
        packed[i] = coarse
        start_lines(i)

    for side, row in ((0, 0), (1, rows - 1)):
        pn[:, row, :] = fx_n[side]

    for group in (cells_in, kinds_in, layers_in):
        group[1].wait()
    uw_z.wait()
    uw_x.wait()

    def elastic(z, u_up, u_down, w_up, w_down):
        now, before, kind = u[z], w[z], k[z]
        lap_u = laplace(now, u_up, u_down, hx_uw[0, 0, pl.ds(z, 1), :], hx_uw[1, 0, pl.ds(z, 1), :])
        lap_w = laplace(before, w_up, w_down, hx_uw[0, 1, pl.ds(z, 1), :], hx_uw[1, 1, pl.ds(z, 1), :])
        shear, viscosity = jnp.zeros(now.shape, F32), jnp.zeros(now.shape, F32)
        for i in range(kinds):
            shear = jnp.where(kind == i, layers[0, i], shear)
            viscosity = jnp.where(kind == i, layers[1, i], viscosity)
        mid = 2.0 * now - before + shear * lap_u + viscosity * (lap_u - lap_w)
        um[z] = mid
        fx_e[0, pl.ds(z, 1), :] = mid[:1]
        fx_e[1, pl.ds(z, 1), :] = mid[-1:]
        rest[z] = now + viscosity * lap_u
        both[z] = shear + viscosity

    elastic(0, hz_uw[0, 0], u[1], hz_uw[0, 1], w[1])
    elastic(tile_rows - 1, u[tile_rows - 2], hz_uw[1, 0], w[tile_rows - 2], hz_uw[1, 1])
    lax.fori_loop(1, tile_rows - 1, lambda z, carry: (
        elastic(z, u[z - 1], u[z + 1], w[z - 1], w[z + 1]), carry)[1], 0)

    cells = tile_rows * tile_cols

    def landings():
        spread = -(-blocks * slots // 128)
        sources = jnp.concatenate([got[0, :, capacity, :]] * spread, axis=1)[:, :blocks * slots]
        mine = iota((blocks, blocks * slots), 1) // slots == iota((blocks, blocks * slots), 0)
        spots = jnp.sum(jnp.where(mine, sources, 0.0), axis=0, keepdims=True) - 1.0

        def landing_of(cell):
            return jnp.where(cell.astype(F32) == spots, 1.0, 0.0).astype(BF16)

        landing = landing_of(iota((cells, blocks * slots), 0))
        edges = 2 * tile_cols + 2 * tile_rows
        edge = iota((edges, blocks * slots), 0)
        beyond = edge - 2 * tile_cols
        edge_landing = landing_of(jnp.where(
            edge < tile_cols, edge, jnp.where(
                edge < 2 * tile_cols, edge + (cells - 2 * tile_cols), jnp.where(
                    beyond < tile_rows, beyond * tile_cols, (beyond - tile_rows) * tile_cols + tile_cols - 1))))
        real = lax.rem(iota((blocks * slots, half), 0), slots) < capacity
        return landing, edge_landing, real

    chunk = 4 if tile_rows % 4 == 0 else 1
    for i in range(chunks):
        at = depths(i)
        all_lines[i].wait_recv()
        if i == 0:
            landing, edge_landing, real = landings()
        lines = jnp.where(real, got[i].reshape(blocks * slots, half), 0.0)
        parts = jnp.concatenate(split(lines), axis=1)

        def sums(where):
            result = dot(where, parts)
            return result[:, :half] + result[:, half:]

        edge_force = 0.25 * sums(edge_landing)
        for side, z in ((0, 0), (1, tile_rows - 1)):
            fz_e[side, :, at] = um[z, :, at] + edge_force[side * tile_cols:(side + 1) * tile_cols]
            here = 2 * tile_cols + side * tile_rows
            fx_e[side, :, at] = fx_e[side, :, at] + edge_force[here:here + tile_rows]
        e_x.start(i)
        e_z.start(i)
        for r in range(0, tile_rows, chunk):
            force = sums(landing[r * tile_cols:(r + chunk) * tile_cols]).reshape(chunk, tile_cols, half)
            tf[r:r + chunk, :, at] = force
            um[r:r + chunk, :, at] = um[r:r + chunk, :, at] + 0.25 * force

    def final(z, up, down):
        now = um[z]
        un[z] = 2.0 * now - rest[z] + both[z] * laplace(now, up, down) + 0.25 * tf[z]

    final(0, None, um[1])
    final(tile_rows - 1, um[tile_rows - 2], None)
    lax.fori_loop(1, tile_rows - 1, lambda z, carry: (final(z, um[z - 1], um[z + 1]), carry)[1], 0, unroll=2)

    for item in all_lines:
        item.wait_send()
    e_z.wait()
    e_x.wait()
    hz_out[...] = hz_e[...]
    hx_out[...] = hx_e[...]
    along_gx.wait_sent(paired, 2 * rows + 3 * tile_cols * tile_depth // lateral)
    along_gy.wait_sent(paired, 2 * planes + 3 * tile_rows * tile_depth // lateral)


def finish(pm, pn, tf, um, partial, both, hz, hx, pm_out, pn_out, tf_out, um_out, un_out, un, sems):
    copies = [pltpu.make_async_copy(s, d, sems.at[i]) for i, (s, d) in enumerate(
        ((pm, pm_out), (pn, pn_out), (tf, tf_out), (um, um_out)))]
    for copy in copies:
        copy.start()
    tile_rows, tile_cols, _ = um.shape

    def final(z, carry):
        scale = both[z]
        row = iota(scale.shape, 0)
        extra = jnp.where(row == 0, hx[0, pl.ds(z, 1), :], 0.0) + jnp.where(
            row == tile_cols - 1, hx[1, pl.ds(z, 1), :], 0.0)
        un[z] = partial[z] + scale * extra
        return carry

    lax.fori_loop(0, tile_rows, final, 0)
    for side, z in ((0, 0), (1, tile_rows - 1)):
        un[z] = un[z] + both[z] * hz[side]
    copies.append(pltpu.make_async_copy(un, un_out, sems.at[4]))
    copies[4].start()
    for copy in copies:
        copy.wait()


def local(pressure, pressure_prev, courant, nonlinearity, absorption, own_map, slot_table,
          displacement, displacement_prev, layer_labels, shear_table, viscosity_table):
    planes, rows, lateral = pressure.shape
    tile = displacement.shape
    blocks = lax.axis_size("gx") * lax.axis_size("gy")
    capacity = max(2, own_map.shape[0] * own_map.shape[1] // blocks)
    slots = -(-(capacity + 1) // 8) * 8
    width = 256
    chunks = lateral // width
    hbm = pl.BlockSpec(memory_space=pltpu.HBM)
    vmem = pl.BlockSpec(memory_space=pltpu.VMEM)
    wave, cell = pltpu.VMEM(pressure.shape, F32), pltpu.VMEM(tile, F32)

    def along_z(shape):
        return pltpu.VMEM((2,) + shape[1:], F32)

    def along_x(shape):
        return pltpu.VMEM((2, shape[0], shape[2]), F32)

    dma, regular = pltpu.SemaphoreType.DMA, pltpu.SemaphoreType.REGULAR
    kinds = shear_table.shape[0]
    wave_z, wave_x, cell_z, cell_x = along_z(pressure.shape), along_x(pressure.shape), along_z(tile), along_x(tile)
    lines = pltpu.VMEM((chunks, blocks, slots, width // 2), F32)
    waves = [jax.ShapeDtypeStruct(pressure.shape, F32)] * 2
    cells = [jax.ShapeDtypeStruct(tile, F32)]
    parts = pl.pallas_call(
        functools.partial(kernel, capacity, slots, width),
        out_shape=[wave] * 2 + [cell] * 4 + [cell_z, cell_x],
        in_specs=[hbm] * 12,
        out_specs=[vmem] * 8,
        scratch_shapes=[
            pltpu.VMEM((5,) + pressure.shape, F32), pltpu.VMEM((2,) + tile, F32), pltpu.VMEM(tile, jnp.int32),
            pltpu.VMEM((2,) + own_map.shape[::-1], jnp.int32), pltpu.SMEM((2, kinds), F32), dma((12,)),
            pltpu.VMEM((2 * (planes + rows), lateral), F32), pltpu.VMEM((4, planes, lateral), F32),
            wave_x, wave_x, cell_z, cell_x,
            wave_z, wave_x, wave_z, wave_x,
            pltpu.VMEM((2, 2) + tile[1:], F32), pltpu.VMEM((2, 2, tile[0], tile[2]), F32), cell_z, cell_x,
            cell, pltpu.VMEM((planes // 2 * rows + 2 * planes, lateral), F32), wave_x, lines, lines,
            dma((2,)), dma((2,)), dma((4 * chunks + 4,)), dma((chunks,)), dma((chunks,)), regular((2,)), regular((2,))],
        compiler_params=pltpu.CompilerParams(
            collective_id=0, has_side_effects=True, vmem_limit_bytes=58 * 1024 * 1024),
    )(pressure, pressure_prev, courant, nonlinearity, absorption, own_map.T, slot_table.T,
      displacement, displacement_prev, layer_labels, shear_table, viscosity_table)
    return pl.pallas_call(
        finish,
        out_shape=waves + cells * 3,
        in_specs=[vmem] * 8,
        out_specs=[hbm] * 5,
        scratch_shapes=[cell, dma((5,))],
        compiler_params=pltpu.CompilerParams(vmem_limit_bytes=40 * 1024 * 1024),
    )(*parts)


def solution(mesh):
    field = P(("group", "gx"), "gy", None)
    table = P(("group", "gx"), "gy")
    return jax.shard_map(
        local,
        mesh=mesh,
        in_specs=(field,) * 5 + (table,) * 2 + (field,) * 3 + (P("group"),) * 2,
        out_specs=(field,) * 5,
        check_vma=False,
    )
```

```python
import functools

import jax
import jax.numpy as jnp
from jax import lax
from jax.experimental import pallas as pl
from jax.experimental.pallas import tpu as pltpu
from jax.sharding import PartitionSpec as P

MESH = pl.DeviceIdType.MESH
F32 = jnp.float32
BF16 = jnp.bfloat16


def iota(shape, dim):
    return lax.broadcasted_iota(jnp.int32, shape, dim)


def split(x):
    high = x.astype(BF16)
    low = (x - high.astype(F32)).astype(BF16)
    return high, low


def dot(a, b):
    return jnp.dot(a, b, preferred_element_type=F32)


def laplace(centre, up, down, left=0.0, right=0.0):
    rows, lanes = centre.shape
    row, lane = iota(centre.shape, 0), iota(centre.shape, 1)
    xm = jnp.where(row == 0, left, pltpu.roll(centre, 1, 0))
    xp = jnp.where(row == rows - 1, right, pltpu.roll(centre, rows - 1, 0))
    ym = jnp.where(lane == 0, 0.0, pltpu.roll(centre, 1, 1))
    yp = jnp.where(lane == lanes - 1, 0.0, pltpu.roll(centre, lanes - 1, 1))
    if up is None:
        beside = down
    elif down is None:
        beside = up
    else:
        beside = up + down
    return (beside + (xm + xp)) + ((ym + yp) - 6.0 * centre)


class Faces:
    def __init__(self, line, pieces, halo, recv, base, together=False):
        self.line, self.halo = line, halo
        self.up, self.down, self.one, self.two = [], [], [], []
        for i, (first, last, part) in enumerate(pieces):
            arrived = recv.at[base if together else base + i]
            self.up.append(line.copy(last, part(halo, 0), arrived, True))
            self.down.append(line.copy(first, part(halo, 1), arrived, False))
        parts = [lambda halo, side: halo.at[side]] if together else [part for _, _, part in pieces]
        for i, part in enumerate(parts):
            arrived = recv.at[base + i]
            self.one.append(line.copy(part(halo, 0), part(halo, 0), arrived, True))
            self.two.append(line.copy(part(halo, slice(None)), part(halo, slice(None)), arrived, True))

    def clear(self):
        @pl.when(jnp.logical_not(self.line.has_prev))
        def _():
            self.halo[0] = jnp.zeros(self.halo.shape[1:], F32)

        @pl.when(jnp.logical_not(self.line.has_next))
        def _():
            self.halo[1] = jnp.zeros(self.halo.shape[1:], F32)

    def start(self, i=0):
        pl.when(self.line.has_next)(self.up[i].start)
        pl.when(self.line.has_prev)(self.down[i].start)

    def wait(self, i=0):
        pl.when(self.line.inside)(self.two[i].wait_recv)
        pl.when(self.line.at_end)(self.one[i].wait_recv)


class Line:
    def __init__(self, axis, sent, token):
        size, self.index = lax.axis_size(axis), lax.axis_index(axis)
        index = self.index
        self.size, self.axis, self.sent, self.token = size, axis, sent, token
        self.next = jnp.where(index == size - 1, 0, index + 1)
        self.prev = jnp.where(index == 0, size - 1, index - 1)
        self.has_next, self.has_prev = index < size - 1, index > 0
        self.inside = self.has_next & self.has_prev
        self.at_end = (index == 0) | (index == size - 1)
        self.low = index < size // 2
        self.neighbours = jnp.where(index < size - 1, 1, 0) + jnp.where(index > 0, 1, 0)

    def copy(self, source, target, arrived, up):
        return pltpu.make_async_remote_copy(
            src_ref=source, dst_ref=target, send_sem=self.sent.at[0 if up else 1], recv_sem=arrived,
            device_id={self.axis: self.next if up else self.prev}, device_id_type=MESH)

    def greet(self, barrier):
        for here, other in ((self.has_next, self.next), (self.has_prev, self.prev)):
            @pl.when(here)
            def _():
                pl.semaphore_signal(barrier, inc=1, device_id={self.axis: other}, device_id_type=MESH)

    def tell_next(self):
        pl.semaphore_signal(self.token.at[0], inc=1, device_id={self.axis: self.next}, device_id_type=MESH)

    def tell_prev(self):
        pl.semaphore_signal(self.token.at[1], inc=1, device_id={self.axis: self.prev}, device_id_type=MESH)

    def open(self):
        pl.when(self.index == 0)(self.tell_next)
        pl.when(self.index == self.size - 1)(self.tell_prev)

    def pass_up(self, where):
        @pl.when(where & self.inside)
        def _():
            pl.semaphore_wait(self.token.at[0], 1)
            self.tell_next()

    def pass_down(self, where):
        @pl.when(where & self.inside)
        def _():
            pl.semaphore_wait(self.token.at[1], 1)
            self.tell_prev()

    def near(self):
        self.pass_up(self.low)
        self.pass_down(jnp.logical_not(self.low))

    def far(self):
        self.pass_up(jnp.logical_not(self.low))
        self.pass_down(self.low)

    def close(self):
        @pl.when(self.index == 0)
        def _():
            pl.semaphore_wait(self.token.at[1], 1)

        @pl.when(self.index == self.size - 1)
        def _():
            pl.semaphore_wait(self.token.at[0], 1)

    def wait_sent(self, ref, size):
        whole = ref.at[0:size]
        pl.when(self.has_next)(self.copy(whole, whole, self.sent.at[0], True).wait_send)
        pl.when(self.has_prev)(self.copy(whole, whole, self.sent.at[0], False).wait_send)


def kernel(
    capacity, slots, width,
    p_in, q_in, c_in, n_in, a_in, own_in, slot_in, u_in, w_in, k_in, shear_in, viscosity_in,
    pm, pn, tf, um, un, both, hz_out, hx_out,
    fields, now_before, k, tables, layers, load,
    faces_p, sides, fx_m, fx_n, fz_e, fx_e,
    hz_p, hx_p, hz_m, hx_m, hz_uw, hx_uw, hz_e, hx_e,
    rest, paired, gain, packed, got,
    sent_z, sent_x, recv, line_send, line_recv, token_z, token_x,
):
    _, planes, rows, lateral = fields.shape
    _, tile_rows, tile_cols, tile_depth = now_before.shape
    kinds = layers.shape[1]
    p, q, c, n, a = (fields.at[i] for i in range(5))
    u, w = now_before.at[0], now_before.at[1]
    own, slot = tables.at[0], tables.at[1]
    fx_p = [faces_p.at[i * planes:(i + 1) * planes] for i in range(2)]
    fz_p = [faces_p.at[2 * planes + i * rows:2 * planes + (i + 1) * rows] for i in range(2)]
    fx_c, fx_a = sides.at[0:2], sides.at[2:4]
    half = width // 2
    chunks = lateral // width
    gx, gy = lax.axis_size("gx"), lax.axis_size("gy")
    blocks = gx * gy
    me_x, me_y = lax.axis_index("gx"), lax.axis_index("gy")
    me = me_x * gy + me_y
    along_gx, along_gy = Line("gx", sent_z, token_z), Line("gy", sent_x, token_x)

    barrier = pltpu.get_barrier_semaphore()
    cuts = 3 if planes % 3 == 0 else 1
    step = planes // cuts

    def loads(at, total, pairs):
        copies = [pltpu.make_async_copy(s, d, load.at[at]) for s, d in pairs]
        return copies, pltpu.make_async_copy(total, total, load.at[at])

    def start(group):
        for copy in group[0]:
            copy.start()

    faces_in = loads(0, faces_p, (
        (p_in.at[:, 0, :], fx_p[0]), (p_in.at[:, rows - 1, :], fx_p[1]),
        (p_in.at[0], fz_p[0]), (p_in.at[planes - 1], fz_p[1])))
    waves_in = []
    for i in range(cuts):
        part = pl.ds(i * step, step)
        waves_in.append(loads(6 + i, fields.at[:, part], [
            (s.at[part], fields.at[j, part]) for j, s in enumerate((p_in, q_in, c_in, n_in, a_in))]))
    tables_in = loads(1, tables, ((own_in, own), (slot_in, slot)))
    sides_in = loads(2, sides, (
        (c_in.at[:, 0, :], sides.at[0]), (c_in.at[:, rows - 1, :], sides.at[1]),
        (a_in.at[:, 0, :], sides.at[2]), (a_in.at[:, rows - 1, :], sides.at[3])))
    cells_in = loads(3, now_before, ((u_in, u), (w_in, w)))
    kinds_in = loads(4, k, ((k_in, k),))
    layers_in = loads(5, layers, ((shear_in, layers.at[0]), (viscosity_in, layers.at[1])))

    along_gx.greet(barrier)
    along_gy.greet(barrier)
    for group in [faces_in] + waves_in + [sides_in, tables_in, cells_in, kinds_in, layers_in]:
        start(group)

    def lanes(i):
        return slice(i * width, (i + 1) * width)

    def depths(i):
        return slice(i * half, (i + 1) * half)

    def cut_all(first, last, at):
        def part(where):
            return lambda halo, side: halo.at[side, :, where]
        return [(first.at[:, at(i)], last.at[:, at(i)], part(at(i))) for i in range(chunks)]

    def both_of(first, last):
        return [(f, l, lambda halo, side, i=i: halo.at[side, i]) for i, (f, l) in enumerate(zip(first, last))]

    p_z = Faces(along_gx, cut_all(*fz_p, lanes), hz_p, recv, 0)
    p_x = Faces(along_gy, cut_all(*fx_p, lanes), hx_p, recv, chunks)
    m_z = Faces(along_gx, cut_all(pm.at[0], pm.at[planes - 1], lanes), hz_m, recv, 2 * chunks)
    m_x = Faces(along_gy, cut_all(fx_m.at[0], fx_m.at[1], lanes), hx_m, recv, 3 * chunks)
    at = 4 * chunks
    e_z = Faces(along_gx, cut_all(fz_e.at[0], fz_e.at[1], depths), hz_e, recv, 2 * chunks, True)
    e_x = Faces(along_gy, cut_all(fx_e.at[0], fx_e.at[1], depths), hx_e, recv, 3 * chunks, True)
    uw_z = Faces(along_gx, both_of(
        (u_in.at[0], w_in.at[0]), (u_in.at[tile_rows - 1], w_in.at[tile_rows - 1])), hz_uw, recv, at, True)
    uw_x = Faces(along_gy, both_of(
        (u_in.at[:, 0, :], w_in.at[:, 0, :]),
        (u_in.at[:, tile_cols - 1, :], w_in.at[:, tile_cols - 1, :])), hx_uw, recv, at + 1, True)

    faces_in[1].wait()
    pl.semaphore_wait(barrier, along_gx.neighbours + along_gy.neighbours)
    for i in range(chunks):
        p_x.start(i)
        p_z.start(i)
    along_gx.open()
    for item in (p_z, p_x, m_z, m_x, uw_z, uw_x, e_z, e_x):
        item.clear()

    def wave(now, before, lap, z):
        return (2.0 * now - before + c[z] * lap + n[z] * (now * now - before * before)
                - 0.1 * a[z] * (now - before))

    def first(z, up, down):
        now = p[z]
        mid = wave(now, q[z], laplace(now, up, down), z)
        pm[z] = mid
        fx_m[0, pl.ds(z, 1), :] = mid[:1]
        fx_m[1, pl.ds(z, 1), :] = mid[-1:]

    for i, group in enumerate(waves_in):
        group[1].wait()
        low, high = i * step - 1, (i + 1) * step - 1
        if i == 0:
            first(0, None, p[1])
            low = 1
        if i == cuts - 1:
            high = planes - 1
        lax.fori_loop(low, high, lambda z, carry: (first(z, p[z - 1], p[z + 1]), carry)[1], 0, unroll=2)
        if i == cuts - 1:
            first(planes - 1, p[planes - 2], None)
        if i == 0:
            along_gx.near()
        if i == min(1, cuts - 1):
            along_gx.far()
        if i == cuts - 1:
            along_gx.close()
            along_gy.open()
    sides_in[1].wait()

    tables_in[1].wait()
    lines_x, lines_z = own.shape
    count = lines_z * rows
    total = count + 2 * planes
    padded = -(-total // 128) * 128

    def line_of(column):
        beyond = column - count
        side = jnp.where(beyond >= planes, 1, 0)
        x = jnp.where(column < count, lax.rem(column, rows) // 2, side * (lines_x - 1))
        z = jnp.where(column < count, column // rows, (beyond - side * planes) // 2)
        return z, x

    def along_lanes(table):
        z_of, x_of = line_of(iota((lines_x, padded), 1))
        here = x_of == iota((lines_x, padded), 0)
        result = jnp.zeros((lines_x, padded), F32)
        for z in range(lines_z):
            result = result + jnp.where(here & (z_of == z), table[:, z:z + 1], 0.0)
        return jnp.sum(result, axis=0, keepdims=True)

    owners = own[...].astype(F32)
    owner_lane = along_lanes(owners)
    owner_row = jnp.transpose(jnp.broadcast_to(owner_lane, (128, padded)))[:count, :1]
    owner_lane = owner_lane[:, :total]
    place_lane = along_lanes(slot[...].astype(F32))[:, :total]
    z_of, x_of = line_of(iota((count, total), 1))
    earlier = iota((count, total), 0) // 2 < z_of * lines_x + x_of
    rank = 0.5 * jnp.sum(
        jnp.where((owner_row == owner_lane) & earlier, 1.0, 0.0), axis=0, keepdims=True)
    target = owner_lane * float(slots) + rank
    match = iota((blocks * slots, total), 0).astype(F32) == target
    column = iota((blocks * slots, total), 1)
    counted = (lax.rem(column, 2) == 0) & (column < count)
    places = jnp.sum(jnp.where(match & counted, place_lane + 1.0, 0.0), axis=1, keepdims=True)
    aligned = lax.rem(iota((blocks * slots, 128), 0), slots) == lax.rem(iota((blocks * slots, 128), 1), slots)
    places = jnp.where(aligned, places, 0.0).reshape(blocks, slots, 128)
    places = jnp.sum(places, axis=1, keepdims=True)
    match = jnp.where(match, 1.0, 0.0).astype(BF16)

    for i in range(chunks):
        at = lanes(i)
        p_x.wait(i)
        p_z.wait(i)
        top = c[0, :, at] * hz_p[0, :, at]
        bottom = c[planes - 1, :, at] * hz_p[1, :, at]
        pm[0, :, at] = pm[0, :, at] + top
        pm[planes - 1, :, at] = pm[planes - 1, :, at] + bottom
        z = iota((planes, width), 0)
        for side, row in ((0, 0), (1, rows - 1)):
            extra = sides[side, :, at] * hx_p[side, :, at]
            extra = extra + jnp.where(z == 0, top[row:row + 1], 0.0)
            extra = extra + jnp.where(z == planes - 1, bottom[row:row + 1], 0.0)
            mid = fx_m[side, :, at] + extra
            fx_m[side, :, at] = mid
            pm[:, row, at] = mid
        m_x.start(i)
        m_z.start(i)
    for item in (uw_x, uw_z):
        item.start(0)
        item.start(1)
    along_gy.near()

    def second(z, up, down):
        now = pm[z]
        new = wave(now, p[z], laplace(now, up, down), z)
        pn[z] = new
        fx_n[0, pl.ds(z, 1), :] = new[:1]
        fx_n[1, pl.ds(z, 1), :] = new[-1:]
        return 0.1 * a[z] * (now * now + new * new) * lax.rsqrt(c[z])

    def pair_at(i):
        return pl.ds(pl.multiple_of(i * rows, rows), rows)

    paired[pair_at(0), :] = second(0, None, pm[1]) + second(1, pm[0], pm[2])
    last = planes // 2 - 1

    def two(i, carry):
        z = 2 * i
        paired[pair_at(i), :] = second(z, pm[z - 1], pm[z + 1]) + second(z + 1, pm[z], pm[z + 2])
        return carry

    middle = last // 2 + 1
    lax.fori_loop(1, middle, two, 0)
    along_gy.far()
    lax.fori_loop(middle, last, two, 0)
    paired[pair_at(last), :] = second(planes - 2, pm[planes - 3], pm[planes - 1]) + second(
        planes - 1, pm[planes - 2], None)
    gain[...] = 0.1 * sides[2:4] * lax.rsqrt(sides[0:2])

    used = [pl.ds(0, capacity + 1)] + [pl.ds(0, capacity)] * (chunks - 1)
    others = pl.ds(0, blocks - 1)

    def line_copy(i, source, target_ref, x, y):
        return pltpu.make_async_remote_copy(
            src_ref=source, dst_ref=target_ref, send_sem=line_send.at[i], recv_sem=line_recv.at[i],
            device_id={"gx": x, "gy": y}, device_id_type=MESH)

    def turn(index, by, size):
        moved = index + by
        return jnp.where(moved >= size, moved - size, moved)

    far_first = sorted(range(gy), key=lambda by: -min(by, gy - by))
    xs, ys = [turn(me_x, by, gx) for by in range(gx)], [turn(me_y, by, gy) for by in range(gy)]

    def start_lines(i):
        def send(x, y):
            other = x * gy + y
            line_copy(i, packed.at[i, other, used[i]], got.at[i, me, used[i]], x, y).start()

        if blocks <= 32:
            for by in far_first:
                for ax in range(gx):
                    if by or ax:
                        send(xs[ax], ys[by])
        else:
            def one(d, carry):
                other = lax.rem(me + d, blocks)
                send(other // gy, lax.rem(other, gy))
                return carry

            lax.fori_loop(1, blocks, one, 0)
        got[i, me] = packed[i, me]

    all_lines = [line_copy(
        i, packed.at[i, others, used[i]], got.at[i, others, used[i]], me_x, me_y) for i in range(chunks)]

    lanes_two = jnp.where(iota((width, half), 0) // 2 == iota((width, half), 1), 0.125, 0.0).astype(BF16)
    for i in range(chunks):
        at = lanes(i)
        m_x.wait(i)
        m_z.wait(i)
        for side, z, pair in ((0, 0, 0), (1, planes - 1, last)):
            old = pn[z, :, at]
            extra = c[z, :, at] * hz_m[side, :, at]
            new = old + extra
            pn[z, :, at] = new
            fx_n[0, z:z + 1, at] = new[:1]
            fx_n[1, z:z + 1, at] = new[-1:]
            where = slice(pair * rows, (pair + 1) * rows)
            paired[where, at] = paired[where, at] + (
                0.1 * a[z, :, at] * lax.rsqrt(c[z, :, at]) * (extra * (2.0 * old + extra)))
        for side in range(2):
            old = fx_n[side, :, at]
            extra = sides[side, :, at] * hx_m[side, :, at]
            fx_n[side, :, at] = old + extra
            paired[count + side * planes:count + (side + 1) * planes, at] = (
                gain[side, :, at] * (extra * (2.0 * old + extra)))
        high, low = split(paired[:, at])
        coarse = dot(high, lanes_two) + dot(low, lanes_two)
        high, low = split(coarse)
        coarse = (dot(match, high) + dot(match, low)).reshape(blocks, slots, half)
        if i == 0:
            coarse = jnp.where(iota(coarse.shape, 1) == capacity, places, coarse)
            along_gy.close()
        packed[i] = coarse
        start_lines(i)

    for side, row in ((0, 0), (1, rows - 1)):
        pn[:, row, :] = fx_n[side]

    for group in (cells_in, kinds_in, layers_in):
        group[1].wait()
    uw_z.wait()
    uw_x.wait()

    def elastic(z, u_up, u_down, w_up, w_down):
        now, before, kind = u[z], w[z], k[z]
        lap_u = laplace(now, u_up, u_down, hx_uw[0, 0, pl.ds(z, 1), :], hx_uw[1, 0, pl.ds(z, 1), :])
        lap_w = laplace(before, w_up, w_down, hx_uw[0, 1, pl.ds(z, 1), :], hx_uw[1, 1, pl.ds(z, 1), :])
        shear, viscosity = jnp.zeros(now.shape, F32), jnp.zeros(now.shape, F32)
        for i in range(kinds):
            shear = jnp.where(kind == i, layers[0, i], shear)
            viscosity = jnp.where(kind == i, layers[1, i], viscosity)
        mid = 2.0 * now - before + shear * lap_u + viscosity * (lap_u - lap_w)
        um[z] = mid
        fx_e[0, pl.ds(z, 1), :] = mid[:1]
        fx_e[1, pl.ds(z, 1), :] = mid[-1:]
        rest[z] = now + viscosity * lap_u
        both[z] = shear + viscosity

    elastic(0, hz_uw[0, 0], u[1], hz_uw[0, 1], w[1])
    elastic(tile_rows - 1, u[tile_rows - 2], hz_uw[1, 0], w[tile_rows - 2], hz_uw[1, 1])
    lax.fori_loop(1, tile_rows - 1, lambda z, carry: (
        elastic(z, u[z - 1], u[z + 1], w[z - 1], w[z + 1]), carry)[1], 0)

    cells = tile_rows * tile_cols

    def landings():
        spread = -(-blocks * slots // 128)
        sources = jnp.concatenate([got[0, :, capacity, :]] * spread, axis=1)[:, :blocks * slots]
        mine = iota((blocks, blocks * slots), 1) // slots == iota((blocks, blocks * slots), 0)
        spots = jnp.sum(jnp.where(mine, sources, 0.0), axis=0, keepdims=True) - 1.0

        def landing_of(cell):
            return jnp.where(cell.astype(F32) == spots, 1.0, 0.0).astype(BF16)

        landing = landing_of(iota((cells, blocks * slots), 0))
        edges = 2 * tile_cols + 2 * tile_rows
        edge = iota((edges, blocks * slots), 0)
        beyond = edge - 2 * tile_cols
        edge_landing = landing_of(jnp.where(
            edge < tile_cols, edge, jnp.where(
                edge < 2 * tile_cols, edge + (cells - 2 * tile_cols), jnp.where(
                    beyond < tile_rows, beyond * tile_cols, (beyond - tile_rows) * tile_cols + tile_cols - 1))))
        real = lax.rem(iota((blocks * slots, half), 0), slots) < capacity
        return landing, edge_landing, real

    chunk = 4 if tile_rows % 4 == 0 else 1
    for i in range(chunks):
        at = depths(i)
        all_lines[i].wait_recv()
        if i == 0:
            landing, edge_landing, real = landings()
        lines = jnp.where(real, got[i].reshape(blocks * slots, half), 0.0)
        parts = jnp.concatenate(split(lines), axis=1)

        def sums(where):
            result = dot(where, parts)
            return result[:, :half] + result[:, half:]

        edge_force = 0.25 * sums(edge_landing)
        for side, z in ((0, 0), (1, tile_rows - 1)):
            fz_e[side, :, at] = um[z, :, at] + edge_force[side * tile_cols:(side + 1) * tile_cols]
            here = 2 * tile_cols + side * tile_rows
            fx_e[side, :, at] = fx_e[side, :, at] + edge_force[here:here + tile_rows]
        e_x.start(i)
        e_z.start(i)
        for r in range(0, tile_rows, chunk):
            force = sums(landing[r * tile_cols:(r + chunk) * tile_cols]).reshape(chunk, tile_cols, half)
            tf[r:r + chunk, :, at] = force
            um[r:r + chunk, :, at] = um[r:r + chunk, :, at] + 0.25 * force

    def final(z, up, down):
        now = um[z]
        un[z] = 2.0 * now - rest[z] + both[z] * laplace(now, up, down) + 0.25 * tf[z]

    final(0, None, um[1])
    final(tile_rows - 1, um[tile_rows - 2], None)
    lax.fori_loop(1, tile_rows - 1, lambda z, carry: (final(z, um[z - 1], um[z + 1]), carry)[1], 0, unroll=2)

    for item in all_lines:
        item.wait_send()
    e_z.wait()
    e_x.wait()
    hz_out[...] = hz_e[...]
    hx_out[...] = hx_e[...]
    along_gx.wait_sent(paired, 2 * rows + 3 * tile_cols * tile_depth // lateral)
    along_gy.wait_sent(paired, 2 * planes + 3 * tile_rows * tile_depth // lateral)


def finish(pm, pn, tf, um, partial, both, hz, hx, pm_out, pn_out, tf_out, um_out, un_out, un, sems):
    copies = [pltpu.make_async_copy(s, d, sems.at[i]) for i, (s, d) in enumerate(
        ((pm, pm_out), (pn, pn_out), (tf, tf_out), (um, um_out)))]
    for copy in copies:
        copy.start()
    tile_rows, tile_cols, _ = um.shape

    def final(z, carry):
        scale = both[z]
        row = iota(scale.shape, 0)
        extra = jnp.where(row == 0, hx[0, pl.ds(z, 1), :], 0.0) + jnp.where(
            row == tile_cols - 1, hx[1, pl.ds(z, 1), :], 0.0)
        un[z] = partial[z] + scale * extra
        return carry

    lax.fori_loop(0, tile_rows, final, 0)
    for side, z in ((0, 0), (1, tile_rows - 1)):
        un[z] = un[z] + both[z] * hz[side]
    copies.append(pltpu.make_async_copy(un, un_out, sems.at[4]))
    copies[4].start()
    for copy in copies:
        copy.wait()


def local(pressure, pressure_prev, courant, nonlinearity, absorption, own_map, slot_table,
          displacement, displacement_prev, layer_labels, shear_table, viscosity_table):
    planes, rows, lateral = pressure.shape
    tile = displacement.shape
    blocks = lax.axis_size("gx") * lax.axis_size("gy")
    capacity = max(2, own_map.shape[0] * own_map.shape[1] // blocks)
    slots = -(-(capacity + 1) // 8) * 8
    width = 256
    chunks = lateral // width
    hbm = pl.BlockSpec(memory_space=pltpu.HBM)
    vmem = pl.BlockSpec(memory_space=pltpu.VMEM)
    wave, cell = pltpu.VMEM(pressure.shape, F32), pltpu.VMEM(tile, F32)

    def along_z(shape):
        return pltpu.VMEM((2,) + shape[1:], F32)

    def along_x(shape):
        return pltpu.VMEM((2, shape[0], shape[2]), F32)

    dma, regular = pltpu.SemaphoreType.DMA, pltpu.SemaphoreType.REGULAR
    kinds = shear_table.shape[0]
    wave_z, wave_x, cell_z, cell_x = along_z(pressure.shape), along_x(pressure.shape), along_z(tile), along_x(tile)
    lines = pltpu.VMEM((chunks, blocks, slots, width // 2), F32)
    waves = [jax.ShapeDtypeStruct(pressure.shape, F32)] * 2
    cells = [jax.ShapeDtypeStruct(tile, F32)]
    parts = pl.pallas_call(
        functools.partial(kernel, capacity, slots, width),
        out_shape=[wave] * 2 + [cell] * 4 + [cell_z, cell_x],
        in_specs=[hbm] * 12,
        out_specs=[vmem] * 8,
        scratch_shapes=[
            pltpu.VMEM((5,) + pressure.shape, F32), pltpu.VMEM((2,) + tile, F32), pltpu.VMEM(tile, jnp.int32),
            pltpu.VMEM((2,) + own_map.shape[::-1], jnp.int32), pltpu.SMEM((2, kinds), F32), dma((9,)),
            pltpu.VMEM((2 * (planes + rows), lateral), F32), pltpu.VMEM((4, planes, lateral), F32),
            wave_x, wave_x, cell_z, cell_x,
            wave_z, wave_x, wave_z, wave_x,
            pltpu.VMEM((2, 2) + tile[1:], F32), pltpu.VMEM((2, 2, tile[0], tile[2]), F32), cell_z, cell_x,
            cell, pltpu.VMEM((planes // 2 * rows + 2 * planes, lateral), F32), wave_x, lines, lines,
            dma((2,)), dma((2,)), dma((4 * chunks + 2,)), dma((chunks,)), dma((chunks,)), regular((2,)), regular((2,))],
        compiler_params=pltpu.CompilerParams(
            collective_id=0, has_side_effects=True, vmem_limit_bytes=58 * 1024 * 1024),
    )(pressure, pressure_prev, courant, nonlinearity, absorption, own_map.T, slot_table.T,
      displacement, displacement_prev, layer_labels, shear_table, viscosity_table)
    return pl.pallas_call(
        finish,
        out_shape=waves + cells * 3,
        in_specs=[vmem] * 8,
        out_specs=[hbm] * 5,
        scratch_shapes=[cell, dma((5,))],
        compiler_params=pltpu.CompilerParams(vmem_limit_bytes=40 * 1024 * 1024),
    )(*parts)


def solution(mesh):
    field = P(("group", "gx"), "gy", None)
    table = P(("group", "gx"), "gy")
    return jax.shard_map(
        local,
        mesh=mesh,
        in_specs=(field,) * 5 + (table,) * 2 + (field,) * 3 + (P("group"),) * 2,
        out_specs=(field,) * 5,
        check_vma=False,
    )
```

```python
import functools

import jax
import jax.numpy as jnp
from jax import lax
from jax.experimental import pallas as pl
from jax.experimental.pallas import tpu as pltpu
from jax.sharding import PartitionSpec as P

MESH = pl.DeviceIdType.MESH
F32 = jnp.float32
BF16 = jnp.bfloat16


def iota(shape, dim):
    return lax.broadcasted_iota(jnp.int32, shape, dim)


def split(x):
    high = x.astype(BF16)
    low = (x - high.astype(F32)).astype(BF16)
    return high, low


def dot(a, b):
    return jnp.dot(a, b, preferred_element_type=F32)


def laplace(centre, up, down, left=0.0, right=0.0):
    rows, lanes = centre.shape
    row, lane = iota(centre.shape, 0), iota(centre.shape, 1)
    xm = jnp.where(row == 0, left, pltpu.roll(centre, 1, 0))
    xp = jnp.where(row == rows - 1, right, pltpu.roll(centre, rows - 1, 0))
    ym = jnp.where(lane == 0, 0.0, pltpu.roll(centre, 1, 1))
    yp = jnp.where(lane == lanes - 1, 0.0, pltpu.roll(centre, lanes - 1, 1))
    if up is None:
        beside = down
    elif down is None:
        beside = up
    else:
        beside = up + down
    return (beside + (xm + xp)) + ((ym + yp) - 6.0 * centre)


class Faces:
    def __init__(self, line, pieces, halo, recv, base, together=False):
        self.line, self.halo = line, halo
        self.up, self.down, self.one, self.two = [], [], [], []
        for i, (first, last, part) in enumerate(pieces):
            arrived = recv.at[base if together else base + i]
            self.up.append(line.copy(last, part(halo, 0), arrived, True))
            self.down.append(line.copy(first, part(halo, 1), arrived, False))
        parts = [lambda halo, side: halo.at[side]] if together else [part for _, _, part in pieces]
        for i, part in enumerate(parts):
            arrived = recv.at[base + i]
            self.one.append(line.copy(part(halo, 0), part(halo, 0), arrived, True))
            self.two.append(line.copy(part(halo, slice(None)), part(halo, slice(None)), arrived, True))

    def clear(self):
        @pl.when(jnp.logical_not(self.line.has_prev))
        def _():
            self.halo[0] = jnp.zeros(self.halo.shape[1:], F32)

        @pl.when(jnp.logical_not(self.line.has_next))
        def _():
            self.halo[1] = jnp.zeros(self.halo.shape[1:], F32)

    def start(self, i=0):
        pl.when(self.line.has_next)(self.up[i].start)
        pl.when(self.line.has_prev)(self.down[i].start)

    def wait(self, i=0):
        pl.when(self.line.inside)(self.two[i].wait_recv)
        pl.when(self.line.at_end)(self.one[i].wait_recv)


class Line:
    def __init__(self, axis, sent, token):
        size, self.index = lax.axis_size(axis), lax.axis_index(axis)
        index = self.index
        self.size, self.axis, self.sent, self.token = size, axis, sent, token
        self.next = jnp.where(index == size - 1, 0, index + 1)
        self.prev = jnp.where(index == 0, size - 1, index - 1)
        self.has_next, self.has_prev = index < size - 1, index > 0
        self.inside = self.has_next & self.has_prev
        self.at_end = (index == 0) | (index == size - 1)
        self.low = index < size // 2
        self.neighbours = jnp.where(index < size - 1, 1, 0) + jnp.where(index > 0, 1, 0)

    def copy(self, source, target, arrived, up):
        return pltpu.make_async_remote_copy(
            src_ref=source, dst_ref=target, send_sem=self.sent.at[0 if up else 1], recv_sem=arrived,
            device_id={self.axis: self.next if up else self.prev}, device_id_type=MESH)

    def greet(self, barrier):
        for here, other in ((self.has_next, self.next), (self.has_prev, self.prev)):
            @pl.when(here)
            def _():
                pl.semaphore_signal(barrier, inc=1, device_id={self.axis: other}, device_id_type=MESH)

    def tell_next(self):
        pl.semaphore_signal(self.token.at[0], inc=1, device_id={self.axis: self.next}, device_id_type=MESH)

    def tell_prev(self):
        pl.semaphore_signal(self.token.at[1], inc=1, device_id={self.axis: self.prev}, device_id_type=MESH)

    def open(self):
        pl.when(self.index == 0)(self.tell_next)
        pl.when(self.index == self.size - 1)(self.tell_prev)

    def pass_up(self, where):
        @pl.when(where & self.inside)
        def _():
            pl.semaphore_wait(self.token.at[0], 1)
            self.tell_next()

    def pass_down(self, where):
        @pl.when(where & self.inside)
        def _():
            pl.semaphore_wait(self.token.at[1], 1)
            self.tell_prev()

    def near(self):
        self.pass_up(self.low)
        self.pass_down(jnp.logical_not(self.low))

    def far(self):
        self.pass_up(jnp.logical_not(self.low))
        self.pass_down(self.low)

    def close(self):
        @pl.when(self.index == 0)
        def _():
            pl.semaphore_wait(self.token.at[1], 1)

        @pl.when(self.index == self.size - 1)
        def _():
            pl.semaphore_wait(self.token.at[0], 1)

    def wait_sent(self, ref, size):
        whole = ref.at[0:size]
        pl.when(self.has_next)(self.copy(whole, whole, self.sent.at[0], True).wait_send)
        pl.when(self.has_prev)(self.copy(whole, whole, self.sent.at[0], False).wait_send)


def kernel(
    capacity, slots, width,
    p_in, q_in, c_in, n_in, a_in, own_in, slot_in, u_in, w_in, k_in, shear_in, viscosity_in,
    pm, pn, tf, um, un, both, hz_out, hx_out,
    fields, now_before, k, tables, layers, load,
    faces_p, sides, fx_m, fx_n, fz_e, fx_e,
    hz_p, hx_p, hz_m, hx_m, hz_uw, hx_uw, hz_e, hx_e,
    rest, paired, gain, gain_z, packed, got,
    sent_z, sent_x, recv, line_send, line_recv, token_z, token_x,
):
    _, planes, rows, lateral = fields.shape
    _, tile_rows, tile_cols, tile_depth = now_before.shape
    kinds = layers.shape[1]
    p, q, c, n, a = (fields.at[i] for i in range(5))
    u, w = now_before.at[0], now_before.at[1]
    own, slot = tables.at[0], tables.at[1]
    fx_p = [faces_p.at[i * planes:(i + 1) * planes] for i in range(2)]
    fz_p = [faces_p.at[2 * planes + i * rows:2 * planes + (i + 1) * rows] for i in range(2)]
    fx_c, fx_a = sides.at[0:2], sides.at[2:4]
    half = width // 2
    chunks = lateral // width
    gx, gy = lax.axis_size("gx"), lax.axis_size("gy")
    blocks = gx * gy
    me_x, me_y = lax.axis_index("gx"), lax.axis_index("gy")
    me = me_x * gy + me_y
    along_gx, along_gy = Line("gx", sent_z, token_z), Line("gy", sent_x, token_x)

    barrier = pltpu.get_barrier_semaphore()
    cuts = 3 if planes % 3 == 0 else 1
    step = planes // cuts

    def loads(at, total, pairs):
        copies = [pltpu.make_async_copy(s, d, load.at[at]) for s, d in pairs]
        return copies, pltpu.make_async_copy(total, total, load.at[at])

    def start(group):
        for copy in group[0]:
            copy.start()

    faces_in = loads(0, faces_p, (
        (p_in.at[:, 0, :], fx_p[0]), (p_in.at[:, rows - 1, :], fx_p[1]),
        (p_in.at[0], fz_p[0]), (p_in.at[planes - 1], fz_p[1])))
    waves_in = []
    for i in range(cuts):
        part = pl.ds(i * step, step)
        waves_in.append(loads(6 + i, fields.at[:, part], [
            (s.at[part], fields.at[j, part]) for j, s in enumerate((p_in, q_in, c_in, n_in, a_in))]))
    tables_in = loads(1, tables, ((own_in, own), (slot_in, slot)))
    sides_in = loads(2, sides, (
        (c_in.at[:, 0, :], sides.at[0]), (c_in.at[:, rows - 1, :], sides.at[1]),
        (a_in.at[:, 0, :], sides.at[2]), (a_in.at[:, rows - 1, :], sides.at[3])))
    cells_in = loads(3, now_before, ((u_in, u), (w_in, w)))
    kinds_in = loads(4, k, ((k_in, k),))
    layers_in = loads(5, layers, ((shear_in, layers.at[0]), (viscosity_in, layers.at[1])))

    along_gx.greet(barrier)
    along_gy.greet(barrier)
    for group in [faces_in] + waves_in + [sides_in, tables_in, cells_in, kinds_in, layers_in]:
        start(group)

    def lanes(i):
        return slice(i * width, (i + 1) * width)

    def depths(i):
        return slice(i * half, (i + 1) * half)

    def cut_all(first, last, at):
        def part(where):
            return lambda halo, side: halo.at[side, :, where]
        return [(first.at[:, at(i)], last.at[:, at(i)], part(at(i))) for i in range(chunks)]

    def both_of(first, last):
        return [(f, l, lambda halo, side, i=i: halo.at[side, i]) for i, (f, l) in enumerate(zip(first, last))]

    p_z = Faces(along_gx, cut_all(*fz_p, lanes), hz_p, recv, 0)
    p_x = Faces(along_gy, cut_all(*fx_p, lanes), hx_p, recv, chunks)
    m_z = Faces(along_gx, cut_all(pm.at[0], pm.at[planes - 1], lanes), hz_m, recv, 2 * chunks)
    m_x = Faces(along_gy, cut_all(fx_m.at[0], fx_m.at[1], lanes), hx_m, recv, 3 * chunks)
    at = 4 * chunks
    e_z = Faces(along_gx, cut_all(fz_e.at[0], fz_e.at[1], depths), hz_e, recv, at, True)
    e_x = Faces(along_gy, cut_all(fx_e.at[0], fx_e.at[1], depths), hx_e, recv, at + 1, True)
    uw_z = Faces(along_gx, both_of(
        (u_in.at[0], w_in.at[0]), (u_in.at[tile_rows - 1], w_in.at[tile_rows - 1])), hz_uw, recv, at + 2, True)
    uw_x = Faces(along_gy, both_of(
        (u_in.at[:, 0, :], w_in.at[:, 0, :]),
        (u_in.at[:, tile_cols - 1, :], w_in.at[:, tile_cols - 1, :])), hx_uw, recv, at + 3, True)

    faces_in[1].wait()
    pl.semaphore_wait(barrier, along_gx.neighbours + along_gy.neighbours)
    for i in range(chunks):
        p_x.start(i)
        p_z.start(i)
    along_gx.open()
    for item in (p_z, p_x, m_z, m_x, uw_z, uw_x, e_z, e_x):
        item.clear()

    def wave(now, before, lap, z):
        return (2.0 * now - before + c[z] * lap + n[z] * (now * now - before * before)
                - 0.1 * a[z] * (now - before))

    def first(z, up, down):
        now = p[z]
        mid = wave(now, q[z], laplace(now, up, down), z)
        pm[z] = mid
        fx_m[0, pl.ds(z, 1), :] = mid[:1]
        fx_m[1, pl.ds(z, 1), :] = mid[-1:]

    for i, group in enumerate(waves_in):
        group[1].wait()
        low, high = i * step - 1, (i + 1) * step - 1
        if i == 0:
            first(0, None, p[1])
            low = 1
        if i == cuts - 1:
            high = planes - 1
        lax.fori_loop(low, high, lambda z, carry: (first(z, p[z - 1], p[z + 1]), carry)[1], 0, unroll=2)
        if i == cuts - 1:
            first(planes - 1, p[planes - 2], None)
        if i == 0:
            along_gx.near()
        if i == min(1, cuts - 1):
            along_gx.far()
        if i == cuts - 1:
            along_gx.close()
            along_gy.open()
    sides_in[1].wait()

    tables_in[1].wait()
    lines_x, lines_z = own.shape
    count = lines_z * rows
    total = count + 2 * planes
    padded = -(-total // 128) * 128

    def line_of(column):
        beyond = column - count
        side = jnp.where(beyond >= planes, 1, 0)
        x = jnp.where(column < count, lax.rem(column, rows) // 2, side * (lines_x - 1))
        z = jnp.where(column < count, column // rows, (beyond - side * planes) // 2)
        return z, x

    def along_lanes(table):
        z_of, x_of = line_of(iota((lines_x, padded), 1))
        here = x_of == iota((lines_x, padded), 0)
        result = jnp.zeros((lines_x, padded), F32)
        for z in range(lines_z):
            result = result + jnp.where(here & (z_of == z), table[:, z:z + 1], 0.0)
        return jnp.sum(result, axis=0, keepdims=True)

    owners = own[...].astype(F32)
    owner_lane = along_lanes(owners)
    owner_row = jnp.transpose(jnp.broadcast_to(owner_lane, (128, padded)))[:count, :1]
    owner_lane = owner_lane[:, :total]
    place_lane = along_lanes(slot[...].astype(F32))[:, :total]
    z_of, x_of = line_of(iota((count, total), 1))
    earlier = iota((count, total), 0) // 2 < z_of * lines_x + x_of
    rank = 0.5 * jnp.sum(
        jnp.where((owner_row == owner_lane) & earlier, 1.0, 0.0), axis=0, keepdims=True)
    target = owner_lane * float(slots) + rank
    match = iota((blocks * slots, total), 0).astype(F32) == target
    column = iota((blocks * slots, total), 1)
    counted = (lax.rem(column, 2) == 0) & (column < count)
    places = jnp.sum(jnp.where(match & counted, place_lane + 1.0, 0.0), axis=1, keepdims=True)
    aligned = lax.rem(iota((blocks * slots, 128), 0), slots) == lax.rem(iota((blocks * slots, 128), 1), slots)
    places = jnp.where(aligned, places, 0.0).reshape(blocks, slots, 128)
    places = jnp.sum(places, axis=1, keepdims=True)
    match = jnp.where(match, 1.0, 0.0).astype(BF16)

    for i in range(chunks):
        at = lanes(i)
        p_x.wait(i)
        p_z.wait(i)
        top = c[0, :, at] * hz_p[0, :, at]
        bottom = c[planes - 1, :, at] * hz_p[1, :, at]
        pm[0, :, at] = pm[0, :, at] + top
        pm[planes - 1, :, at] = pm[planes - 1, :, at] + bottom
        z = iota((planes, width), 0)
        for side, row in ((0, 0), (1, rows - 1)):
            extra = sides[side, :, at] * hx_p[side, :, at]
            extra = extra + jnp.where(z == 0, top[row:row + 1], 0.0)
            extra = extra + jnp.where(z == planes - 1, bottom[row:row + 1], 0.0)
            mid = fx_m[side, :, at] + extra
            fx_m[side, :, at] = mid
            pm[:, row, at] = mid
        m_x.start(i)
        m_z.start(i)
    for item in (uw_x, uw_z):
        item.start(0)
        item.start(1)
    along_gy.near()

    def second(z, up, down):
        now = pm[z]
        new = wave(now, p[z], laplace(now, up, down), z)
        pn[z] = new
        fx_n[0, pl.ds(z, 1), :] = new[:1]
        fx_n[1, pl.ds(z, 1), :] = new[-1:]
        return 0.1 * a[z] * (now * now + new * new) * lax.rsqrt(c[z])

    def pair_at(i):
        return pl.ds(pl.multiple_of(i * rows, rows), rows)

    paired[pair_at(0), :] = second(0, None, pm[1]) + second(1, pm[0], pm[2])
    last = planes // 2 - 1

    def two(i, carry):
        z = 2 * i
        paired[pair_at(i), :] = second(z, pm[z - 1], pm[z + 1]) + second(z + 1, pm[z], pm[z + 2])
        return carry

    middle = last // 2 + 1
    lax.fori_loop(1, middle, two, 0)
    along_gy.far()
    lax.fori_loop(middle, last, two, 0)
    paired[pair_at(last), :] = second(planes - 2, pm[planes - 3], pm[planes - 1]) + second(
        planes - 1, pm[planes - 2], None)
    gain[...] = 0.1 * sides[2:4] * lax.rsqrt(sides[0:2])
    for side, z in ((0, 0), (1, planes - 1)):
        gain_z[side] = 0.1 * a[z] * lax.rsqrt(c[z])

    used = [pl.ds(0, capacity + 1)] + [pl.ds(0, capacity)] * (chunks - 1)
    others = pl.ds(0, blocks - 1)

    def line_copy(i, source, target_ref, x, y):
        return pltpu.make_async_remote_copy(
            src_ref=source, dst_ref=target_ref, send_sem=line_send.at[i], recv_sem=line_recv.at[i],
            device_id={"gx": x, "gy": y}, device_id_type=MESH)

    def turn(index, by, size):
        moved = index + by
        return jnp.where(moved >= size, moved - size, moved)

    far_first = sorted(range(gy), key=lambda by: -min(by, gy - by))
    xs, ys = [turn(me_x, by, gx) for by in range(gx)], [turn(me_y, by, gy) for by in range(gy)]

    def start_lines(i):
        def send(x, y):
            other = x * gy + y
            line_copy(i, packed.at[i, other, used[i]], got.at[i, me, used[i]], x, y).start()

        if blocks <= 32:
            for by in far_first:
                for ax in range(gx):
                    if by or ax:
                        send(xs[ax], ys[by])
        else:
            def one(d, carry):
                other = lax.rem(me + d, blocks)
                send(other // gy, lax.rem(other, gy))
                return carry

            lax.fori_loop(1, blocks, one, 0)
        got[i, me] = packed[i, me]

    all_lines = [line_copy(
        i, packed.at[i, others, used[i]], got.at[i, others, used[i]], me_x, me_y) for i in range(chunks)]

    lanes_two = jnp.where(iota((width, half), 0) // 2 == iota((width, half), 1), 0.125, 0.0).astype(BF16)
    for i in range(chunks):
        at = lanes(i)
        m_x.wait(i)
        m_z.wait(i)
        for side, z, pair in ((0, 0, 0), (1, planes - 1, last)):
            old = pn[z, :, at]
            extra = c[z, :, at] * hz_m[side, :, at]
            new = old + extra
            pn[z, :, at] = new
            fx_n[0, z:z + 1, at] = new[:1]
            fx_n[1, z:z + 1, at] = new[-1:]
            where = slice(pair * rows, (pair + 1) * rows)
            paired[where, at] = paired[where, at] + (
                gain_z[side, :, at] * (extra * (2.0 * old + extra)))
        for side in range(2):
            old = fx_n[side, :, at]
            extra = sides[side, :, at] * hx_m[side, :, at]
            fx_n[side, :, at] = old + extra
            paired[count + side * planes:count + (side + 1) * planes, at] = (
                gain[side, :, at] * (extra * (2.0 * old + extra)))
        high, low = split(paired[:, at])
        coarse = dot(high, lanes_two) + dot(low, lanes_two)
        coarse = dot(match, jnp.concatenate(split(coarse), axis=1))
        coarse = (coarse[:, :half] + coarse[:, half:]).reshape(blocks, slots, half)
        if i == 0:
            coarse = jnp.where(iota(coarse.shape, 1) == capacity, places, coarse)
            along_gy.close()
        packed[i] = coarse
        start_lines(i)

    for side, row in ((0, 0), (1, rows - 1)):
        pn[:, row, :] = fx_n[side]

    for group in (cells_in, kinds_in, layers_in):
        group[1].wait()
    uw_z.wait()
    uw_x.wait()

    def elastic(z, u_up, u_down, w_up, w_down):
        now, before, kind = u[z], w[z], k[z]
        lap_u = laplace(now, u_up, u_down, hx_uw[0, 0, pl.ds(z, 1), :], hx_uw[1, 0, pl.ds(z, 1), :])
        lap_w = laplace(before, w_up, w_down, hx_uw[0, 1, pl.ds(z, 1), :], hx_uw[1, 1, pl.ds(z, 1), :])
        shear, viscosity = jnp.zeros(now.shape, F32), jnp.zeros(now.shape, F32)
        for i in range(kinds):
            shear = jnp.where(kind == i, layers[0, i], shear)
            viscosity = jnp.where(kind == i, layers[1, i], viscosity)
        mid = 2.0 * now - before + shear * lap_u + viscosity * (lap_u - lap_w)
        um[z] = mid
        fx_e[0, pl.ds(z, 1), :] = mid[:1]
        fx_e[1, pl.ds(z, 1), :] = mid[-1:]
        rest[z] = now + viscosity * lap_u
        both[z] = shear + viscosity

    elastic(0, hz_uw[0, 0], u[1], hz_uw[0, 1], w[1])
    elastic(tile_rows - 1, u[tile_rows - 2], hz_uw[1, 0], w[tile_rows - 2], hz_uw[1, 1])
    lax.fori_loop(1, tile_rows - 1, lambda z, carry: (
        elastic(z, u[z - 1], u[z + 1], w[z - 1], w[z + 1]), carry)[1], 0)

    cells = tile_rows * tile_cols

    def landings():
        spread = -(-blocks * slots // 128)
        sources = jnp.concatenate([got[0, :, capacity, :]] * spread, axis=1)[:, :blocks * slots]
        mine = iota((blocks, blocks * slots), 1) // slots == iota((blocks, blocks * slots), 0)
        spots = jnp.sum(jnp.where(mine, sources, 0.0), axis=0, keepdims=True) - 1.0

        def landing_of(cell):
            return jnp.where(cell.astype(F32) == spots, 1.0, 0.0).astype(BF16)

        landing = landing_of(iota((cells, blocks * slots), 0))
        edges = 2 * tile_cols + 2 * tile_rows
        edge = iota((edges, blocks * slots), 0)
        beyond = edge - 2 * tile_cols
        edge_landing = landing_of(jnp.where(
            edge < tile_cols, edge, jnp.where(
                edge < 2 * tile_cols, edge + (cells - 2 * tile_cols), jnp.where(
                    beyond < tile_rows, beyond * tile_cols, (beyond - tile_rows) * tile_cols + tile_cols - 1))))
        real = lax.rem(iota((blocks * slots, half), 0), slots) < capacity
        return landing, edge_landing, real

    chunk = 4 if tile_rows % 4 == 0 else 1
    for i in range(chunks):
        at = depths(i)
        all_lines[i].wait_recv()
        if i == 0:
            landing, edge_landing, real = landings()
        lines = jnp.where(real, got[i].reshape(blocks * slots, half), 0.0)
        parts = jnp.concatenate(split(lines), axis=1)

        def sums(where):
            result = dot(where, parts)
            return result[:, :half] + result[:, half:]

        edge_force = 0.25 * sums(edge_landing)
        for side, z in ((0, 0), (1, tile_rows - 1)):
            fz_e[side, :, at] = um[z, :, at] + edge_force[side * tile_cols:(side + 1) * tile_cols]
            here = 2 * tile_cols + side * tile_rows
            fx_e[side, :, at] = fx_e[side, :, at] + edge_force[here:here + tile_rows]
        e_x.start(i)
        e_z.start(i)
        for r in range(0, tile_rows, chunk):
            force = sums(landing[r * tile_cols:(r + chunk) * tile_cols]).reshape(chunk, tile_cols, half)
            tf[r:r + chunk, :, at] = force
            um[r:r + chunk, :, at] = um[r:r + chunk, :, at] + 0.25 * force

    def final(z, up, down):
        now = um[z]
        un[z] = 2.0 * now - rest[z] + both[z] * laplace(now, up, down) + 0.25 * tf[z]

    final(0, None, um[1])
    final(tile_rows - 1, um[tile_rows - 2], None)
    lax.fori_loop(1, tile_rows - 1, lambda z, carry: (final(z, um[z - 1], um[z + 1]), carry)[1], 0, unroll=2)

    for item in all_lines:
        item.wait_send()
    e_z.wait()
    e_x.wait()
    hz_out[...] = hz_e[...]
    hx_out[...] = hx_e[...]
    along_gx.wait_sent(paired, 2 * rows + 3 * tile_cols * tile_depth // lateral)
    along_gy.wait_sent(paired, 2 * planes + 3 * tile_rows * tile_depth // lateral)


def finish(pm, pn, tf, um, partial, both, hz, hx, pm_out, pn_out, tf_out, um_out, un_out, un, sems):
    copies = [pltpu.make_async_copy(s, d, sems.at[i]) for i, (s, d) in enumerate(
        ((pm, pm_out), (pn, pn_out), (tf, tf_out), (um, um_out)))]
    for copy in copies:
        copy.start()
    tile_rows, tile_cols, _ = um.shape

    def final(z, carry):
        scale = both[z]
        row = iota(scale.shape, 0)
        extra = jnp.where(row == 0, hx[0, pl.ds(z, 1), :], 0.0) + jnp.where(
            row == tile_cols - 1, hx[1, pl.ds(z, 1), :], 0.0)
        un[z] = partial[z] + scale * extra
        return carry

    lax.fori_loop(0, tile_rows, final, 0)
    for side, z in ((0, 0), (1, tile_rows - 1)):
        un[z] = un[z] + both[z] * hz[side]
    copies.append(pltpu.make_async_copy(un, un_out, sems.at[4]))
    copies[4].start()
    for copy in copies:
        copy.wait()


def local(pressure, pressure_prev, courant, nonlinearity, absorption, own_map, slot_table,
          displacement, displacement_prev, layer_labels, shear_table, viscosity_table):
    planes, rows, lateral = pressure.shape
    tile = displacement.shape
    blocks = lax.axis_size("gx") * lax.axis_size("gy")
    capacity = max(2, own_map.shape[0] * own_map.shape[1] // blocks)
    slots = -(-(capacity + 1) // 8) * 8
    width = 256
    chunks = lateral // width
    hbm = pl.BlockSpec(memory_space=pltpu.HBM)
    vmem = pl.BlockSpec(memory_space=pltpu.VMEM)
    wave, cell = pltpu.VMEM(pressure.shape, F32), pltpu.VMEM(tile, F32)

    def along_z(shape):
        return pltpu.VMEM((2,) + shape[1:], F32)

    def along_x(shape):
        return pltpu.VMEM((2, shape[0], shape[2]), F32)

    dma, regular = pltpu.SemaphoreType.DMA, pltpu.SemaphoreType.REGULAR
    kinds = shear_table.shape[0]
    wave_z, wave_x, cell_z, cell_x = along_z(pressure.shape), along_x(pressure.shape), along_z(tile), along_x(tile)
    lines = pltpu.VMEM((chunks, blocks, slots, width // 2), F32)
    waves = [jax.ShapeDtypeStruct(pressure.shape, F32)] * 2
    cells = [jax.ShapeDtypeStruct(tile, F32)]
    parts = pl.pallas_call(
        functools.partial(kernel, capacity, slots, width),
        out_shape=[wave] * 2 + [cell] * 4 + [cell_z, cell_x],
        in_specs=[hbm] * 12,
        out_specs=[vmem] * 8,
        scratch_shapes=[
            pltpu.VMEM((5,) + pressure.shape, F32), pltpu.VMEM((2,) + tile, F32), pltpu.VMEM(tile, jnp.int32),
            pltpu.VMEM((2,) + own_map.shape[::-1], jnp.int32), pltpu.SMEM((2, kinds), F32), dma((9,)),
            pltpu.VMEM((2 * (planes + rows), lateral), F32), pltpu.VMEM((4, planes, lateral), F32),
            wave_x, wave_x, cell_z, cell_x,
            wave_z, wave_x, wave_z, wave_x,
            pltpu.VMEM((2, 2) + tile[1:], F32), pltpu.VMEM((2, 2, tile[0], tile[2]), F32), cell_z, cell_x,
            cell, pltpu.VMEM((planes // 2 * rows + 2 * planes, lateral), F32), wave_x, wave_z, lines, lines,
            dma((2,)), dma((2,)), dma((4 * chunks + 4,)), dma((chunks,)), dma((chunks,)), regular((2,)), regular((2,))],
        compiler_params=pltpu.CompilerParams(
            collective_id=0, has_side_effects=True, vmem_limit_bytes=58 * 1024 * 1024),
    )(pressure, pressure_prev, courant, nonlinearity, absorption, own_map.T, slot_table.T,
      displacement, displacement_prev, layer_labels, shear_table, viscosity_table)
    return pl.pallas_call(
        finish,
        out_shape=waves + cells * 3,
        in_specs=[vmem] * 8,
        out_specs=[hbm] * 5,
        scratch_shapes=[cell, dma((5,))],
        compiler_params=pltpu.CompilerParams(vmem_limit_bytes=40 * 1024 * 1024),
    )(*parts)


def solution(mesh):
    field = P(("group", "gx"), "gy", None)
    table = P(("group", "gx"), "gy")
    return jax.shard_map(
        local,
        mesh=mesh,
        in_specs=(field,) * 5 + (table,) * 2 + (field,) * 3 + (P("group"),) * 2,
        out_specs=(field,) * 5,
        check_vma=False,
    )
```
